128 devices in a mesh: dp: 8 (over x, core), pp: 16 (over z, y).
Axes of the slice: x: 4, y: 4, z: 4, core: 2. Of those that a mesh axis runs over, the one named last changes fastest.
Arguments:
- hidden: bfloat16 [2048, 4096], P(('dp', 'pp')), may hold values from -400 to 400
- norm_gain: float32 [4096], replicated, may hold values from 0.1 to 1.9
- head: bfloat16 [131072, 4096], P(('dp', 'pp')), may hold values from -32 to 32
- targets: int32 [2048], P(('dp', 'pp')), may hold values from 0 to 131071
- route: int32 [128], replicated, may hold values from 0 to 7
Outputs:
- token_loss: float32 [2048], P(('dp', 'pp'))
- pipe_loss: float32 [8], replicated
The draws below stay inside these ranges and needn't reach their ends.
All inputs are finite; a program needn't handle non-finite values.
Results may differ from the reference program's by a relative error of at most 0.00053.
Values may be sent and summed in bfloat16 or wider, within the bound.
No kernel may reach another device: no remote copies, remote signals or barrier semaphores. Data moves between devices by JAX's collectives and lax.ppermute only.
A program may use at most 64 MiB of HBM per device.

```python
import math
import jax
import jax.numpy as jnp
import numpy as np
from jax import lax

D = 4096
TOK_DEV = 16
VOCAB = 131072
TOKENS = 2048
N_DP = 8
N_PP = 16


def draw_hidden(key, part):
    row_scale = jnp.exp(jax.random.uniform(jax.random.fold_in(key, 11), (TOKENS, 1), jnp.float32, 0.0, 2.302585))
    col_scale = jnp.exp(jax.random.uniform(jax.random.fold_in(key, 12), (1, D), jnp.float32, 0.0, 2.302585))
    base = jnp.clip(jax.random.normal(jax.random.fold_in(key, 13), (TOKENS, D), jnp.float32), -4.0, 4.0)
    base = base * row_scale * col_scale
    return base.astype(jnp.bfloat16)


def draw_head(key, part):
    base = jnp.clip(jax.random.normal(jax.random.fold_in(key, 21), (VOCAB, D), jnp.float32), -4.0, 4.0) * (3.0 / D ** 0.5)
    return base.astype(jnp.bfloat16)


def set_ends(entries, stream_key, low, largest):
    shape = entries.shape
    spot = [jax.random.randint(jax.random.fold_in(stream_key, axis), (), 0, shape[axis]) for axis in range(len(shape))]
    entries = entries.at[tuple(spot)].set(low)
    longest = shape.index(max(shape))
    spot[longest] = (spot[longest] + 1) % shape[longest]
    return entries.at[tuple(spot)].set(largest)


def wide_ids(own_key, extent, count, skew):
    weights = [min(1 << octave, count + 1 - (1 << octave)) * (1 << 20) // math.isqrt((1 << octave) ** skew) + 1 for octave in range((count + 1).bit_length()) if 1 << octave <= count]
    width = 1 + sum(weights) // (1 << 30)
    table = np.cumsum(np.array([max(1, weight // width) for weight in weights]))
    lot = jax.random.randint(jax.random.fold_in(own_key, 1), extent, 0, int(table[len(weights) - 1]))
    start = jnp.left_shift(1, jnp.searchsorted(jnp.asarray(table, jnp.int32), lot, side="right").astype(jnp.int32))
    standing = start - 1 + jax.random.randint(jax.random.fold_in(own_key, 4), extent, 0, 1 << 30) % jnp.minimum(start, count + 1 - start)
    return jax.random.permutation(jax.random.fold_in(own_key, 2), count)[standing].astype(jnp.int32)


def setup_inputs(seed: int = 0) -> dict:
    seeds = jax.random.split(jax.random.key(seed), 6)
    return {
        "hidden": draw_hidden(jax.random.fold_in(seeds[5], 71), 0),
        "norm_gain": jnp.clip(1.0 + 0.18 * jax.random.normal(seeds[1], (D,), jnp.float32), 0.1, 1.9),
        "head": draw_head(jax.random.fold_in(seeds[5], 71), 0),
        "targets": set_ends(wide_ids(seeds[3], (TOKENS,), VOCAB, 2), jax.random.fold_in(seeds[3], 3), 0, VOCAB - 1).astype(jnp.int32),
        "route": set_ends(jax.random.randint(seeds[4], (N_DP * N_PP,), 0, N_DP), jax.random.fold_in(seeds[4], 1), 0, N_DP - 1).astype(jnp.int32),
    }


def rms_normal(rows, gain):
    wide = rows.astype(jnp.float32)
    factor = lax.rsqrt(lax.optimization_barrier(jnp.mean(wide * wide, axis=1, keepdims=True)) + 1e-05)
    return (wide * factor * gain).astype(jnp.bfloat16)

def reference(hidden, norm_gain, head, targets, route):
    normed = rms_normal(hidden, norm_gain)
    block = math.gcd(TOKENS, 512)

    def one_block(pair):
        rows, marks = pair
        logits = lax.dot_general(rows, head, (((1,), (1,)), ((), ())), preferred_element_type=jnp.float32)
        peak = lax.optimization_barrier(jnp.max(logits, axis=1))
        total = peak + jnp.log(lax.optimization_barrier(jnp.sum(jnp.exp(logits - peak[:, None]), axis=1)))
        picked = jnp.take_along_axis(logits, marks[:, None].astype(jnp.int32), axis=1)[:, 0]
        return total - picked
    token_loss = lax.map(one_block, (normed.reshape(TOKENS // block, block, D), targets.reshape(TOKENS // block, block))).reshape(TOKENS)
    per_device = lax.optimization_barrier(jnp.sum(token_loss.reshape(N_DP * N_PP, TOK_DEV), axis=1))
    pick = (route[:, None] == jnp.arange(N_DP, dtype=jnp.int32)[None, :]).astype(jnp.float32)
    pipe_loss = jnp.dot(per_device, pick, precision=lax.Precision.HIGHEST) / (TOKENS // N_DP)
    return (token_loss, pipe_loss)
```

```python
import functools

import jax
import jax.numpy as jnp
from jax import lax
from jax.experimental import pallas as pl
from jax.experimental.pallas import tpu as pltpu
from jax.sharding import Mesh
from jax.sharding import PartitionSpec as P


X, CORE, Z, Y = "dp_0", "dp_1", "pp_0", "pp_1"
ALL = (X, CORE, Z, Y)
CLASS = (X, Z, Y)
RING = 4
OFFSETS = (0, -1, 1, 2)
ORDERS = ((Y, Z, X), (X, Y, Z), (Z, X, Y))
HALF_DIM = (0, 0, 1)
EXTRA = 128
VOCAB_CHUNK = 512


def shift(x, axis, offset):
    return lax.ppermute(x, axis, [(i, (i - offset) % RING) for i in range(RING)])


def norm_kernel(targets, hidden, gain, *parts):
    rows, width = hidden.shape
    wide = hidden[...].astype(jnp.float32)
    factor = lax.rsqrt(jnp.mean(wide * wide, axis=1, keepdims=True) + 1e-05)
    normed = (wide * factor * gain[...]).astype(jnp.bfloat16)
    row = lax.broadcasted_iota(jnp.int32, (rows, EXTRA), 0)
    lane = lax.broadcasted_iota(jnp.int32, (rows, EXTRA), 1)
    ids = jnp.zeros((rows, EXTRA), jnp.int32)
    for i in range(rows):
        ids = jnp.where(row == i, targets[i], ids)
    digit = jnp.where(lane == 0, ids >> 16, jnp.where(lane == 1, (ids >> 8) & 255, ids & 255))
    digit = jnp.where(lane < 3, digit, 0).astype(jnp.float32).astype(jnp.bfloat16)
    part = (width + EXTRA) // 3
    parts[0][...] = normed[:, :part]
    parts[1][...] = normed[:, part : 2 * part]
    parts[2][:, : part - EXTRA] = normed[:, 2 * part :]
    parts[2][:, part - EXTRA :] = digit


def normalize(hidden, gain, targets):
    rows, width = hidden.shape
    part = (width + EXTRA) // 3
    vmem = pl.BlockSpec(memory_space=pltpu.VMEM)
    return pl.pallas_call(
        norm_kernel,
        in_specs=[pl.BlockSpec(memory_space=pltpu.SMEM), vmem, vmem],
        out_specs=[vmem] * 3,
        out_shape=[jax.ShapeDtypeStruct((rows, part), jnp.bfloat16)] * 3,
        name="normalize",
    )(targets, hidden, gain.reshape(1, width))


def in_order(pieces, axis):
    here = lax.axis_index(axis)
    stacked = jnp.zeros((RING,) + pieces[0].shape, pieces[0].dtype)
    for offset, piece in zip(OFFSETS, pieces):
        stacked = lax.dynamic_update_slice_in_dim(stacked, piece[None], (here + offset) % RING, 0)
    return stacked


def gather(parts):
    for phase in range(2):
        moved = [
            [x] + [shift(x, order[phase], offset) for offset in OFFSETS[1:]]
            for x, order in zip(parts, ORDERS)
        ]
        parts = [in_order(m, order[phase]) for m, order in zip(moved, ORDERS)]
    near = [(shift(x, order[2], -1), shift(x, order[2], 1)) for x, order in zip(parts, ORDERS)]
    out = []
    for x, (left, right), order, dim in zip(parts, near, ORDERS, HALF_DIM):
        low = lax.slice_in_dim(left, 0, RING // 2, axis=dim)
        high = lax.slice_in_dim(right, RING // 2, RING, axis=dim)
        out.append((x, left, right, shift(low, order[2], -1), shift(high, order[2], 1)))
    return out


def loss_kernel(place, *refs):
    pieces = [refs[5 * k : 5 * k + 5] for k in range(3)]
    heads = refs[15:17]
    out, rows, vocab, row_sems, head_sems = refs[17:]
    part = pieces[0][0].shape[-1]
    width = heads[0].shape[1]
    shard = pieces[0][0].shape[-2]
    block = RING * RING * shard
    per_head = heads[0].shape[0] // VOCAB_CHUNK
    chunks = 2 * per_head
    half = RING // 2
    at = [[(place[axis] + offset) % RING for offset in OFFSETS] for axis in range(3)]

    def copies(j):
        x = at[0][j]
        sem = row_sems.at[j]
        a, b, c = pieces
        pairs = []
        if j < 3:
            pairs.append((a[j], rows.at[x, :, :, :, :part]))
        else:
            pairs.append((a[3], rows.at[x, :half, :, :, :part]))
            pairs.append((a[4], rows.at[x, half:, :, :, :part]))
        for i in range(3):
            pairs.append((b[i].at[:, x], rows.at[x, at[1][i], :, :, part : 2 * part]))
            pairs.append((c[i].at[x], rows.at[x, :, at[2][i], :, 2 * part :]))
        pairs.append((b[3].at[:, x], rows.at[x, at[1][3], :half, :, part : 2 * part]))
        pairs.append((b[4].at[:, x], rows.at[x, at[1][3], half:, :, part : 2 * part]))
        pairs.append((c[3].at[x], rows.at[x, :half, at[2][3], :, 2 * part :]))
        pairs.append((c[4].at[x], rows.at[x, half:, at[2][3], :, 2 * part :]))
        return [pltpu.make_async_copy(src, dst, sem) for src, dst in pairs]

    def head_copy(c):
        src = heads[c // per_head].at[pl.ds((c % per_head) * VOCAB_CHUNK, VOCAB_CHUNK)]
        return pltpu.make_async_copy(src, vocab.at[c], head_sems.at[c])

    for copy in copies(0):
        copy.start()
    for c in range(chunks):
        head_copy(c).start()
    for j in range(1, RING):
        for copy in copies(j):
            copy.start()

    weight = lax.broadcasted_iota(jnp.int32, (8, EXTRA), 1)
    weight = jnp.where(weight == 0, 65536, jnp.where(weight == 1, 256, jnp.where(weight == 2, 1, 0)))
    weight = weight.astype(jnp.float32).astype(jnp.bfloat16)
    contract = (((1,), (1,)), ((), ()))

    for j in range(RING):
        x = at[0][j]
        pltpu.make_async_copy(rows.at[x], rows.at[x], row_sems.at[j]).wait()
        tokens = rows[x].reshape(block, width + EXTRA)
        label = lax.dot_general(weight, tokens[:, width:], contract, preferred_element_type=jnp.float32)
        label = label[0:1].astype(jnp.int32)
        tokens = tokens[:, :width]
        peak = jnp.full((1, block), -jnp.inf, jnp.float32)
        mass = jnp.zeros((1, block), jnp.float32)
        hit = jnp.zeros((1, block), jnp.float32)
        for c in range(chunks):
            if j == 0:
                head_copy(c).wait()
            logits = lax.dot_general(vocab[c], tokens, contract, preferred_element_type=jnp.float32)
            first = place[3 + c // per_head] + (c % per_head) * VOCAB_CHUNK
            row = lax.broadcasted_iota(jnp.int32, logits.shape, 0)
            hit += jnp.sum(jnp.where(row == label - first, logits, 0.0), axis=0, keepdims=True)
            top = jnp.maximum(peak, jnp.max(logits, axis=0, keepdims=True))
            mass = mass * jnp.exp(peak - top) + jnp.sum(jnp.exp(logits - top), axis=0, keepdims=True)
            peak = top
        total = peak + jnp.log(mass)
        lanes = out.shape[1]
        per_block = block // lanes
        for i in range(per_block):
            out[pl.ds(x * per_block + i, 1), :] = total[:, i * lanes : (i + 1) * lanes]
            out[pl.ds((RING + x) * per_block + i, 1), :] = hit[:, i * lanes : (i + 1) * lanes]


def partial_losses(place, gathered, head, other):
    shard, part = gathered[0][0].shape[-2:]
    count, width = head.shape
    hbm = pl.BlockSpec(memory_space=pltpu.HBM)
    tokens = RING**3 * shard
    chunks = 2 * count // VOCAB_CHUNK
    return pl.pallas_call(
        loss_kernel,
        in_specs=[pl.BlockSpec(memory_space=pltpu.SMEM)] + [hbm] * 17,
        out_specs=pl.BlockSpec(memory_space=pltpu.VMEM),
        out_shape=jax.ShapeDtypeStruct((2 * tokens // 128, 128), jnp.float32),
        scratch_shapes=[
            pltpu.VMEM((RING, RING, RING, shard, 3 * part), jnp.bfloat16),
            pltpu.VMEM((chunks, VOCAB_CHUNK, width), jnp.bfloat16),
            pltpu.SemaphoreType.DMA((RING,)),
            pltpu.SemaphoreType.DMA((chunks,)),
        ],
        compiler_params=pltpu.CompilerParams(vmem_limit_bytes=48 * 1024 * 1024),
        name="partial_losses",
    )(place, *sum(gathered, ()), head, other)


def finish_kernel(mine, stats, pipe_of, losses, pipes):
    half = stats.shape[1] // 2
    lanes = stats.shape[2]
    local = stats[:, :half, :]
    top = jnp.max(local, axis=0)
    mass = jnp.sum(jnp.exp(local - top[None]), axis=0)
    loss = top + jnp.log(mass) - jnp.sum(stats[:, half:, :], axis=0)
    sums = [jnp.sum(jnp.where(pipe_of[...] == p, loss, 0.0), keepdims=True) for p in range(pipes.shape[0])]
    pipes[...] = jnp.concatenate([jnp.broadcast_to(s, (1, lanes)) for s in sums], axis=0)
    row = lax.broadcasted_iota(jnp.int32, loss.shape, 0)
    own = jnp.sum(jnp.where(row == mine[0], loss, 0.0), axis=0, keepdims=True)
    losses[...] = pltpu.roll(own, mine[1], 1)


def finish(mine, stats, pipe_of, pipes):
    vmem = pl.BlockSpec(memory_space=pltpu.VMEM)
    lanes = stats.shape[2]
    return pl.pallas_call(
        finish_kernel,
        in_specs=[pl.BlockSpec(memory_space=pltpu.SMEM), vmem, vmem],
        out_specs=[vmem, vmem],
        out_shape=[
            jax.ShapeDtypeStruct((1, lanes), jnp.float32),
            jax.ShapeDtypeStruct((pipes, lanes), jnp.float32),
        ],
        name="finish",
    )(mine, stats, pipe_of)


def shards(hidden, norm_gain, head, targets, route):
    rows = hidden.shape[0]
    x, core, z, y = (lax.axis_index(a) for a in ALL)
    devices = lax.axis_size(ALL)
    pipes = lax.axis_size((X, CORE))
    count = head.shape[0]
    other = lax.ppermute(head, CORE, [(0, 1), (1, 0)])
    gathered = gather(normalize(hidden, norm_gain, targets))
    own = lax.axis_index(ALL)
    partner = ((x * 2 + 1 - core) * RING + z) * RING + y
    place = jnp.stack([x, z, y, own * count, partner * count]).astype(jnp.int32)
    stats = partial_losses(place, gathered, head, other)
    members = lax.axis_size(CLASS)
    sent = jnp.broadcast_to(stats[None], (members,) + stats.shape)
    stats = lax.all_to_all(sent, CLASS, 0, 0, tiled=True)
    lanes = stats.shape[2]
    member = lax.axis_index(CLASS)
    first = member * rows
    mine = jnp.stack([first // lanes, (lanes - first % lanes) % lanes]).astype(jnp.int32)
    pipe_of = lax.dynamic_index_in_dim(route.reshape(RING, 2, RING * RING), core, 1, keepdims=False)
    pipe_of = jnp.repeat(pipe_of.reshape(members), rows).reshape(members * rows // lanes, lanes)
    losses, sums = finish(mine, stats, pipe_of, pipes)
    sums = sums + lax.ppermute(sums, CORE, [(0, 1), (1, 0)])
    return (losses[0, :rows], sums[:, 0] / (rows * devices // pipes))


def solution(mesh):
    torus = Mesh(mesh.devices.reshape(RING, 2, RING, RING), ALL)
    return jax.shard_map(
        shards,
        mesh=torus,
        in_specs=(P(ALL, None), P(), P(ALL, None), P(ALL), P()),
        out_specs=(P(ALL), P()),
        check_vma=False,
    )
```

```python
import functools

import jax
import jax.numpy as jnp
from jax import lax
from jax.experimental import pallas as pl
from jax.experimental.pallas import tpu as pltpu
from jax.sharding import Mesh
from jax.sharding import PartitionSpec as P


X, CORE, Z, Y = "dp_0", "dp_1", "pp_0", "pp_1"
ALL = (X, CORE, Z, Y)
CLASS = (X, Z, Y)
RING = 4
OFFSETS = (0, -1, 1, 2)
ORDERS = ((Y, Z, X), (X, Y, Z), (Z, X, Y))
EXTRA = 128
VOCAB_CHUNK = 256


def shift(x, axis, offset):
    pairs = []
    for i in range(RING):
        for core in range(2):
            to = (i - offset * (1 - 2 * core)) % RING
            pairs.append((i * 2 + core, to * 2 + core) if axis == X else (core * RING + i, core * RING + to))
    return lax.ppermute(x, (X, CORE) if axis == X else (CORE, axis), pairs)


def sender(axis, offset):
    return (lax.axis_index(axis) + offset * (1 - 2 * lax.axis_index(CORE))) % RING


def norm_kernel(targets, hidden, gain, *parts):
    rows, width = hidden.shape
    wide = hidden[...].astype(jnp.float32)
    factor = lax.rsqrt(jnp.mean(wide * wide, axis=1, keepdims=True) + 1e-05)
    normed = (wide * factor * gain[...]).astype(jnp.bfloat16)
    row = lax.broadcasted_iota(jnp.int32, (rows, EXTRA), 0)
    lane = lax.broadcasted_iota(jnp.int32, (rows, EXTRA), 1)
    ids = jnp.zeros((rows, EXTRA), jnp.int32)
    for i in range(rows):
        ids = jnp.where(row == i, targets[i], ids)
    digit = jnp.where(lane == 0, ids >> 16, jnp.where(lane == 1, (ids >> 8) & 255, ids & 255))
    digit = jnp.where(lane < 3, digit, 0).astype(jnp.float32).astype(jnp.bfloat16)
    part = (width + EXTRA) // 3
    parts[0][...] = normed[:, :part]
    parts[1][...] = normed[:, part : 2 * part]
    parts[2][:, : part - EXTRA] = normed[:, 2 * part :]
    parts[2][:, part - EXTRA :] = digit


def normalize(hidden, gain, targets):
    rows, width = hidden.shape
    part = (width + EXTRA) // 3
    vmem = pl.BlockSpec(memory_space=pltpu.VMEM)
    return pl.pallas_call(
        norm_kernel,
        in_specs=[pl.BlockSpec(memory_space=pltpu.SMEM), vmem, vmem],
        out_specs=[vmem] * 3,
        out_shape=[jax.ShapeDtypeStruct((rows, part), jnp.bfloat16)] * 3,
        name="normalize",
    )(targets, hidden, gain.reshape(1, width))


def in_order(pieces, axis):
    stacked = jnp.zeros((RING,) + pieces[0].shape, pieces[0].dtype)
    for offset, piece in zip(OFFSETS, pieces):
        stacked = lax.dynamic_update_slice_in_dim(stacked, piece[None], sender(axis, offset), 0)
    return stacked


def gather(parts):
    for phase in range(2):
        moved = [
            [x] + [shift(x, order[phase], offset) for offset in OFFSETS[1:]]
            for x, order in zip(parts, ORDERS)
        ]
        parts = [in_order(m, order[phase]) for m, order in zip(moved, ORDERS)]
    near = [[x] + [shift(x, order[2], offset) for offset in OFFSETS[1:3]] for x, order in zip(parts, ORDERS)]
    far = [shift(n[1], order[2], OFFSETS[1]) for n, order in zip(near, ORDERS)]
    return near, far


def head_copies(heads, buffer, sems, step):
    per_head = heads[0].shape[0] // VOCAB_CHUNK
    slot = step % 2
    pairs = []
    for k in range(2):
        start = jnp.clip(step - k * per_head, 0, per_head - 1) * VOCAB_CHUNK
        src = heads[k].at[pl.ds(start, VOCAB_CHUNK)]
        copy = pltpu.make_async_copy(src, buffer.at[slot], sems.at[slot])
        pairs.append((jnp.logical_and(step >= k * per_head, step < (k + 1) * per_head), copy))
    return pairs


def next_head(heads, buffer, sems, step):
    @pl.when(step == 0)
    def _():
        head_copies(heads, buffer, sems, step)[0][1].start()

    for condition, copy in head_copies(heads, buffer, sems, step + 1):
        pl.when(condition)(copy.start)
    head_copies(heads, buffer, sems, step)[0][1].wait()
    return buffer.at[step % 2]


CONTRACT = (((1,), (1,)), ((), ()))


def products(rows, vocab, count):
    part = rows.shape[-1]
    width = vocab.shape[-1]
    out = []
    for k in range(3):
        low, high = k * part, min((k + 1) * part, width)
        tokens = rows[k, :, : high - low]
        out.append(
            lax.dot_general(tokens, vocab[:, low:high], CONTRACT, preferred_element_type=jnp.float32)
        )
    return [[d[i * (d.shape[0] // count) : (i + 1) * (d.shape[0] // count)] for i in range(count)] for d in out]


def add_in(total, k, at, value):
    shard, lanes = total.shape[-2:]
    value = value.reshape(RING, RING, shard, lanes)
    if k == 0:
        total[at] += value
    elif k == 1:
        for x in range(RING):
            total[x, at] += value[:, x]
    else:
        total[:, :, at] += value


def near_kernel(place, *refs):
    pieces, heads, out, rows, vocab, row_sems, head_sems = refs[:9], refs[9:11], *refs[11:]
    step = pl.program_id(0)
    size = rows.shape[1] // 3
    shape = pieces[0].shape

    def copies():
        for k in range(3):
            for i in range(3):
                dst = rows.at[k, pl.ds(i * size, size)]
                src = pieces[3 * k + i]
                yield pltpu.make_async_copy(src, dst, row_sems.at[3 * k + i])

    @pl.when(step == 0)
    def _():
        for copy in copies():
            copy.start()

    vocab = next_head(heads, vocab, head_sems, step)

    @pl.when(step == 0)
    def _():
        for copy in copies():
            copy.wait()

    out[...] = jnp.zeros(out.shape, out.dtype)
    for k, values in enumerate(products(rows, vocab, 3)):
        for i, value in enumerate(values):
            add_in(out, k, place[4 * k + i], value)


def far_kernel(place, *refs):
    pieces, near, heads, sums, out, rows, vocab, extra, labels, total, peak, mass, hit = (
        refs[:3], refs[3:6], refs[6:8], *refs[8:18],
    )
    row_sems, extra_sems, head_sems = refs[18:]
    step = pl.program_id(0)
    shard, lanes = labels.shape[-2:]

    def copies():
        for k in range(3):
            yield pltpu.make_async_copy(pieces[k], rows.at[k], row_sems.at[k])

    def extra_copies():
        for i, src in enumerate((*near, pieces[2])):
            src = src.at[:, pl.ds(src.shape[1] - EXTRA, EXTRA)]
            yield pltpu.make_async_copy(src, extra.at[i], extra_sems.at[i])

    @pl.when(step == 0)
    def _():
        for copy in (*copies(), *extra_copies()):
            copy.start()

    vocab = next_head(heads, vocab, head_sems, step)

    @pl.when(step == 0)
    def _():
        for copy in (*copies(), *extra_copies()):
            copy.wait()
        weight = lax.broadcasted_iota(jnp.int32, (EXTRA, lanes), 0)
        weight = jnp.where(weight == 0, 65536, jnp.where(weight == 1, 256, jnp.where(weight == 2, 1, 0)))
        weight = weight.astype(jnp.float32).astype(jnp.bfloat16)
        for i in range(RING):
            label = jnp.dot(extra[i], weight, preferred_element_type=jnp.float32)
            labels[:, :, place[8 + i]] = label.astype(jnp.int32).reshape(RING, RING, shard, lanes)
        peak[...] = jnp.full(peak.shape, -jnp.inf, jnp.float32)
        mass[...] = jnp.zeros(mass.shape, jnp.float32)
        hit[...] = jnp.zeros(hit.shape, jnp.float32)

    total[...] = sums[...]
    for k, values in enumerate(products(rows, vocab, 1)):
        add_in(total, k, place[4 * k + 3], values[0])

    per_head = heads[0].shape[0] // VOCAB_CHUNK
    first = jnp.where(step < per_head, place[12], place[13] - per_head * VOCAB_CHUNK) + step * VOCAB_CHUNK
    width = total.shape[-1]
    size = RING * shard
    for x in range(RING):
        for z in range(RING):
            logits = total[x, z].reshape(size, width)
            parts = [logits[:, i * lanes : (i + 1) * lanes] for i in range(width // lanes)]
            label = labels[x, z].reshape(size, lanes) - first
            lane = lax.broadcasted_iota(jnp.int32, (size, lanes), 1)
            old = peak[x, z].reshape(size, lanes)
            top = functools.reduce(jnp.maximum, parts, old)
            found = hit[x, z].reshape(size, lanes)
            left = mass[x, z].reshape(size, lanes) * jnp.exp(old - top)
            for i, value in enumerate(parts):
                left += jnp.exp(value - top)
                found += jnp.where(label == lane + i * lanes, value, 0.0)
            peak[x, z] = top.reshape(RING, shard, lanes)
            mass[x, z] = left.reshape(RING, shard, lanes)
            hit[x, z] = found.reshape(RING, shard, lanes)

    @pl.when(step == pl.num_programs(0) - 1)
    def _():
        row = lax.broadcasted_iota(jnp.int32, (lanes, lanes), 0)
        diagonal = row == lax.broadcasted_iota(jnp.int32, (lanes, lanes), 1)
        count = out.shape[0] // 2
        per = lanes // size
        for g in range(count):
            x, z = divmod(g * per, RING)
            high = peak[x, z : z + per].reshape(lanes, lanes)
            low = mass[x, z : z + per].reshape(lanes, lanes)
            found = hit[x, z : z + per].reshape(lanes, lanes)
            top = jnp.max(high, axis=1, keepdims=True)
            value = top + jnp.log(jnp.sum(low * jnp.exp(high - top), axis=1, keepdims=True))
            found = jnp.sum(found, axis=1, keepdims=True)
            out[g : g + 1, :] = jnp.sum(jnp.where(diagonal, value, 0.0), axis=0, keepdims=True)
            out[count + g : count + g + 1, :] = jnp.sum(jnp.where(diagonal, found, 0.0), axis=0, keepdims=True)


def near_logits(place, pieces, head, other):
    shard, part = pieces[0].shape[-2:]
    count, width = head.shape
    steps = 2 * count // VOCAB_CHUNK
    size = RING * RING * shard
    hbm = pl.BlockSpec(memory_space=pltpu.HBM)
    block = (RING, RING, RING, shard, VOCAB_CHUNK)
    flops = 2 * 9 * size * part * 2 * count
    return pl.pallas_call(
        near_kernel,
        grid=(steps,),
        in_specs=[pl.BlockSpec(memory_space=pltpu.SMEM)] + [hbm] * 11,
        out_specs=pl.BlockSpec(block, lambda v: (0, 0, 0, 0, v)),
        out_shape=jax.ShapeDtypeStruct(block[:-1] + (2 * count,), jnp.float32),
        scratch_shapes=[
            pltpu.VMEM((3, 3 * size, part), jnp.bfloat16),
            pltpu.VMEM((2, VOCAB_CHUNK, width), jnp.bfloat16),
            pltpu.SemaphoreType.DMA((9,)),
            pltpu.SemaphoreType.DMA((2,)),
        ],
        compiler_params=pltpu.CompilerParams(vmem_limit_bytes=40 * 1024 * 1024),
        cost_estimate=pl.CostEstimate(flops=flops, bytes_accessed=32 << 20, transcendentals=0),
        name="near_logits",
    )(place, *[p.reshape(size, part) for p in pieces], head, other)


def far_losses(place, pieces, near, head, other, sums):
    shard, part = pieces[0].shape[-2:]
    count, width = head.shape
    steps = 2 * count // VOCAB_CHUNK
    size = RING * RING * shard
    tokens = RING * size
    hbm = pl.BlockSpec(memory_space=pltpu.HBM)
    grid = (RING, RING, RING, shard)
    return pl.pallas_call(
        far_kernel,
        grid=(steps,),
        in_specs=[pl.BlockSpec(memory_space=pltpu.SMEM)]
        + [hbm] * 8
        + [pl.BlockSpec(grid + (VOCAB_CHUNK,), lambda v: (0, 0, 0, 0, v))],
        out_specs=pl.BlockSpec((2 * tokens // 128, 128), lambda v: (0, 0)),
        out_shape=jax.ShapeDtypeStruct((2 * tokens // 128, 128), jnp.float32),
        scratch_shapes=[
            pltpu.VMEM((3, size, part), jnp.bfloat16),
            pltpu.VMEM((2, VOCAB_CHUNK, width), jnp.bfloat16),
            pltpu.VMEM((RING, size, EXTRA), jnp.bfloat16),
            pltpu.VMEM(grid + (128,), jnp.int32),
            pltpu.VMEM(grid + (VOCAB_CHUNK,), jnp.float32),
            pltpu.VMEM(grid + (128,), jnp.float32),
            pltpu.VMEM(grid + (128,), jnp.float32),
            pltpu.VMEM(grid + (128,), jnp.float32),
            pltpu.SemaphoreType.DMA((3,)),
            pltpu.SemaphoreType.DMA((RING,)),
            pltpu.SemaphoreType.DMA((2,)),
        ],
        compiler_params=pltpu.CompilerParams(vmem_limit_bytes=40 * 1024 * 1024),
        name="far_losses",
    )(place, *[p.reshape(size, part) for p in (*pieces, *near)], head, other, sums)


def finish_kernel(mine, stats, pipe_of, losses, pipes):
    half = stats.shape[1] // 2
    lanes = stats.shape[2]
    local = stats[:, :half, :]
    top = jnp.max(local, axis=0)
    mass = jnp.sum(jnp.exp(local - top[None]), axis=0)
    loss = top + jnp.log(mass) - jnp.sum(stats[:, half:, :], axis=0)
    sums = [jnp.sum(jnp.where(pipe_of[...] == p, loss, 0.0), keepdims=True) for p in range(pipes.shape[0])]
    pipes[...] = jnp.concatenate([jnp.broadcast_to(s, (1, lanes)) for s in sums], axis=0)
    row = lax.broadcasted_iota(jnp.int32, loss.shape, 0)
    own = jnp.sum(jnp.where(row == mine[0], loss, 0.0), axis=0, keepdims=True)
    losses[...] = pltpu.roll(own, mine[1], 1)


def finish(mine, stats, pipe_of, pipes):
    vmem = pl.BlockSpec(memory_space=pltpu.VMEM)
    lanes = stats.shape[2]
    return pl.pallas_call(
        finish_kernel,
        in_specs=[pl.BlockSpec(memory_space=pltpu.SMEM), vmem, vmem],
        out_specs=[vmem, vmem],
        out_shape=[
            jax.ShapeDtypeStruct((1, lanes), jnp.float32),
            jax.ShapeDtypeStruct((pipes, lanes), jnp.float32),
        ],
        name="finish",
    )(mine, stats, pipe_of)


def shards(hidden, norm_gain, head, targets, route):
    rows = hidden.shape[0]
    x, core, z, y = (lax.axis_index(a) for a in ALL)
    devices = lax.axis_size(ALL)
    pipes = lax.axis_size((X, CORE))
    count = head.shape[0]
    other = lax.ppermute(head, CORE, [(0, 1), (1, 0)])
    near, far = gather(normalize(hidden, norm_gain, targets))
    own = lax.axis_index(ALL)
    partner = ((x * 2 + 1 - core) * RING + z) * RING + y
    at = [sender(axis, offset) for axis in (X, Z, Y) for offset in OFFSETS]
    place = jnp.stack([*at, own * count, partner * count]).astype(jnp.int32)
    sums = near_logits(place, sum(near, []), head, other)
    stats = far_losses(place, far, near[2], head, other, sums)
    members = lax.axis_size(CLASS)
    sent = jnp.broadcast_to(stats[None], (members,) + stats.shape)
    stats = lax.all_to_all(sent, CLASS, 0, 0, tiled=True)
    lanes = stats.shape[2]
    member = lax.axis_index(CLASS)
    first = member * rows
    mine = jnp.stack([first // lanes, (lanes - first % lanes) % lanes]).astype(jnp.int32)
    pipe_of = lax.dynamic_index_in_dim(route.reshape(RING, 2, RING * RING), core, 1, keepdims=False)
    pipe_of = jnp.repeat(pipe_of.reshape(members), rows).reshape(members * rows // lanes, lanes)
    losses, sums = finish(mine, stats, pipe_of, pipes)
    sums = sums + lax.ppermute(sums, CORE, [(0, 1), (1, 0)])
    return (losses[0, :rows], sums[:, 0] / (rows * devices // pipes))


def solution(mesh):
    torus = Mesh(mesh.devices.reshape(RING, 2, RING, RING), ALL)
    return jax.shard_map(
        shards,
        mesh=torus,
        in_specs=(P(ALL, None), P(), P(ALL, None), P(ALL), P()),
        out_specs=(P(ALL), P()),
        check_vma=False,
    )
```

```python
import functools

import jax
import jax.numpy as jnp
from jax import lax
from jax.experimental import pallas as pl
from jax.experimental.pallas import tpu as pltpu
from jax.sharding import Mesh
from jax.sharding import PartitionSpec as P


X, CORE, Z, Y = "dp_0", "dp_1", "pp_0", "pp_1"
ALL = (X, CORE, Z, Y)
CLASS = (X, Z, Y)
RING = 4
OFFSETS = (0, -1, 1, 2)
ORDERS = ((Y, Z, X), (X, Y, Z), (Z, X, Y))
EXTRA = 128
VOCAB_CHUNK = 512


def shift(x, axis, offset):
    pairs = []
    for i in range(RING):
        for core in range(2):
            to = (i - offset * (1 - 2 * core)) % RING
            pairs.append((i * 2 + core, to * 2 + core) if axis == X else (core * RING + i, core * RING + to))
    return lax.ppermute(x, (X, CORE) if axis == X else (CORE, axis), pairs)


def sender(axis, offset):
    return (lax.axis_index(axis) + offset * (1 - 2 * lax.axis_index(CORE))) % RING


def norm_kernel(targets, hidden, gain, *parts):
    rows, width = hidden.shape
    wide = hidden[...].astype(jnp.float32)
    factor = lax.rsqrt(jnp.mean(wide * wide, axis=1, keepdims=True) + 1e-05)
    normed = (wide * factor * gain[...]).astype(jnp.bfloat16)
    row = lax.broadcasted_iota(jnp.int32, (rows, EXTRA), 0)
    lane = lax.broadcasted_iota(jnp.int32, (rows, EXTRA), 1)
    ids = jnp.zeros((rows, EXTRA), jnp.int32)
    for i in range(rows):
        ids = jnp.where(row == i, targets[i], ids)
    digit = jnp.where(lane == 0, ids >> 16, jnp.where(lane == 1, (ids >> 8) & 255, ids & 255))
    digit = jnp.where(lane < 3, digit, 0).astype(jnp.float32).astype(jnp.bfloat16)
    part = (width + EXTRA) // 3
    parts[0][...] = normed[:, :part]
    parts[1][...] = normed[:, part : 2 * part]
    parts[2][:, : part - EXTRA] = normed[:, 2 * part :]
    parts[2][:, part - EXTRA :] = digit


def normalize(hidden, gain, targets):
    rows, width = hidden.shape
    part = (width + EXTRA) // 3
    vmem = pl.BlockSpec(memory_space=pltpu.VMEM)
    return pl.pallas_call(
        norm_kernel,
        in_specs=[pl.BlockSpec(memory_space=pltpu.SMEM), vmem, vmem],
        out_specs=[vmem] * 3,
        out_shape=[jax.ShapeDtypeStruct((rows, part), jnp.bfloat16)] * 3,
        name="normalize",
    )(targets, hidden, gain.reshape(1, width))


def swap(x, axis, turn):
    pairs = []
    for i in range(RING):
        for core in range(2):
            to = i ^ 1 if (turn + core) % 2 == 0 else RING - 1 - i
            pairs.append((i * 2 + core, to * 2 + core) if axis == X else (core * RING + i, core * RING + to))
    return lax.ppermute(x, (X, CORE) if axis == X else (CORE, axis), pairs)


def put(pieces, places):
    stacked = jnp.zeros((len(pieces),) + pieces[0].shape, pieces[0].dtype)
    for piece, place in zip(pieces, places):
        stacked = lax.dynamic_update_slice_in_dim(stacked, piece[None], place, 0)
    return stacked


def gather(parts):
    for phase in range(2):
        axes = [order[phase] for order in ORDERS]
        first = [swap(x, axis, 0) for x, axis in zip(parts, axes)]
        pairs = [jnp.stack(two) for two in zip(parts, first)]
        second = [swap(x, axis, 1) for x, axis in zip(pairs, axes)]
        core = lax.axis_index(CORE)
        here = [lax.axis_index(axis) for axis in axes]
        even, odd, across = [h ^ 1 for h in here], [RING - 1 - h for h in here], [h ^ 2 for h in here]
        parts = [
            put([x, f, s[0], s[1]], [h, jnp.where(core == 0, e, o), jnp.where(core == 0, o, e), a])
            for x, f, s, h, e, o, a in zip(parts, first, second, here, even, odd, across)
        ]
    near = [[x] + [shift(x, order[2], offset) for offset in OFFSETS[1:3]] for x, order in zip(parts, ORDERS)]
    far = [shift(n[1], order[2], OFFSETS[1]) for n, order in zip(near, ORDERS)]
    return near, far


def head_copies(heads, buffer, sems, step):
    per_head = heads[0].shape[0] // VOCAB_CHUNK
    slot = step % 2
    pairs = []
    for k in range(2):
        start = jnp.clip(step - k * per_head, 0, per_head - 1) * VOCAB_CHUNK
        src = heads[k].at[pl.ds(start, VOCAB_CHUNK)]
        copy = pltpu.make_async_copy(src, buffer.at[slot], sems.at[slot])
        pairs.append((jnp.logical_and(step >= k * per_head, step < (k + 1) * per_head), copy))
    return pairs


def next_head(heads, buffer, sems, step):
    @pl.when(step == 0)
    def _():
        head_copies(heads, buffer, sems, step)[0][1].start()

    for condition, copy in head_copies(heads, buffer, sems, step + 1):
        pl.when(condition)(copy.start)
    head_copies(heads, buffer, sems, step)[0][1].wait()
    return buffer.at[step % 2]


CONTRACT = (((1,), (1,)), ((), ()))


def products(rows, vocab, count):
    part = rows.shape[-1]
    width = vocab.shape[-1]
    out = []
    for k in range(3):
        low, high = k * part, min((k + 1) * part, width)
        tokens = rows[k, :, : high - low]
        out.append(
            lax.dot_general(tokens, vocab[:, low:high], CONTRACT, preferred_element_type=jnp.float32)
        )
    return [[d[i * (d.shape[0] // count) : (i + 1) * (d.shape[0] // count)] for i in range(count)] for d in out]


def add_in(total, k, at, value):
    shard, lanes = total.shape[-2:]
    value = value.reshape(RING, RING, shard, lanes)
    if k == 0:
        total[at] += value
    elif k == 1:
        for x in range(RING):
            total[x, at] += value[:, x]
    else:
        total[:, :, at] += value


PIPES = 8


def split(x):
    coarse = jnp.floor(x * (1.0 / 256.0)) * 256.0
    return coarse, x - coarse


def near_kernel(place, *refs):
    pieces, heads, out, rows, vocab, row_sems, head_sems = refs[:9], refs[9:11], *refs[11:]
    step = pl.program_id(0)
    size = rows.shape[1] // 3
    shape = pieces[0].shape

    def copies():
        for k in range(3):
            for i in range(3):
                dst = rows.at[k, pl.ds(i * size, size)]
                src = pieces[3 * k + i]
                yield pltpu.make_async_copy(src, dst, row_sems.at[3 * k + i])

    @pl.when(step == 0)
    def _():
        for copy in copies():
            copy.start()

    vocab = next_head(heads, vocab, head_sems, step)

    @pl.when(step == 0)
    def _():
        for copy in copies():
            copy.wait()

    out[...] = jnp.zeros(out.shape, out.dtype)
    for k, values in enumerate(products(rows, vocab, 3)):
        for i, value in enumerate(values):
            add_in(out, k, place[4 * k + i], value)


def far_kernel(place, *refs):
    pieces, near, heads, sums, pipe_of, out, rows, vocab, extra, labels, total, peak, mass, hit = (
        refs[:3], refs[3:6], refs[6:8], *refs[8:19],
    )
    row_sems, extra_sems, head_sems = refs[19:]
    step = pl.program_id(0)
    shard, lanes = labels.shape[-2:]

    def copies():
        for k in range(3):
            yield pltpu.make_async_copy(pieces[k], rows.at[k], row_sems.at[k])

    def extra_copies():
        for i, src in enumerate((*near, pieces[2])):
            src = src.at[:, pl.ds(src.shape[1] - EXTRA, EXTRA)]
            yield pltpu.make_async_copy(src, extra.at[i], extra_sems.at[i])

    @pl.when(step == 0)
    def _():
        for copy in (*copies(), *extra_copies()):
            copy.start()

    vocab = next_head(heads, vocab, head_sems, step)

    @pl.when(step == 0)
    def _():
        for copy in (*copies(), *extra_copies()):
            copy.wait()
        weight = lax.broadcasted_iota(jnp.int32, (EXTRA, lanes), 0)
        weight = jnp.where(weight == 0, 65536, jnp.where(weight == 1, 256, jnp.where(weight == 2, 1, 0)))
        weight = weight.astype(jnp.float32).astype(jnp.bfloat16)
        for i in range(RING):
            label = jnp.dot(extra[i], weight, preferred_element_type=jnp.float32)
            labels[:, :, place[8 + i]] = label.astype(jnp.int32).reshape(RING, RING, shard, lanes)
        peak[...] = jnp.full(peak.shape, -jnp.inf, jnp.float32)
        mass[...] = jnp.zeros(mass.shape, jnp.float32)
        hit[...] = jnp.zeros(hit.shape, jnp.float32)

    total[...] = sums[...]
    for k, values in enumerate(products(rows, vocab, 1)):
        add_in(total, k, place[4 * k + 3], values[0])

    per_head = heads[0].shape[0] // VOCAB_CHUNK
    first = jnp.where(step < per_head, place[12], place[13] - per_head * VOCAB_CHUNK) + step * VOCAB_CHUNK
    width = total.shape[-1]
    size = RING * shard
    for x in range(RING):
        for z in range(RING):
            logits = total[x, z].reshape(size, width)
            parts = [logits[:, i * lanes : (i + 1) * lanes] for i in range(width // lanes)]
            label = labels[x, z].reshape(size, lanes) - first
            lane = lax.broadcasted_iota(jnp.int32, (size, lanes), 1)
            old = peak[x, z].reshape(size, lanes)
            top = functools.reduce(jnp.maximum, parts, old)
            found = hit[x, z].reshape(size, lanes)
            left = mass[x, z].reshape(size, lanes) * jnp.exp(old - top)
            for i, value in enumerate(parts):
                left += jnp.exp(value - top)
                found += jnp.where(label == lane + i * lanes, value, 0.0)
            peak[x, z] = top.reshape(RING, shard, lanes)
            mass[x, z] = left.reshape(RING, shard, lanes)
            hit[x, z] = found.reshape(RING, shard, lanes)

    @pl.when(step == pl.num_programs(0) - 1)
    def _():
        row = lax.broadcasted_iota(jnp.int32, (lanes, lanes), 0)
        diagonal = row == lax.broadcasted_iota(jnp.int32, (lanes, lanes), 1)
        count = pipe_of.shape[0]
        per = lanes // size
        values, founds = [], []
        for g in range(count):
            x, z = divmod(g * per, RING)
            high = peak[x, z : z + per].reshape(lanes, lanes)
            low = mass[x, z : z + per].reshape(lanes, lanes)
            found = hit[x, z : z + per].reshape(lanes, lanes)
            top = jnp.max(high, axis=1, keepdims=True)
            value = top + jnp.log(jnp.sum(low * jnp.exp(high - top), axis=1, keepdims=True))
            found = jnp.sum(found, axis=1, keepdims=True)
            values.append(jnp.sum(jnp.where(diagonal, value, 0.0), axis=0, keepdims=True))
            founds.append(jnp.sum(jnp.where(diagonal, found, 0.0), axis=0, keepdims=True))
        found = jnp.concatenate(founds, axis=0)
        coarse, fine = split(found)
        lane = lax.broadcasted_iota(jnp.int32, (1, lanes), 1)
        tail = jnp.zeros((1, lanes), jnp.float32)
        for p in range(PIPES):
            mine = pipe_of[...] == p
            for k, part in enumerate((coarse, fine)):
                value = jnp.sum(jnp.where(mine, part, 0.0), keepdims=True)
                tail = jnp.where(lane == shard + k * PIPES + p, value, tail)
        members = out.shape[0]
        for k in range(lanes // shard):
            rolled = found if k == 0 else pltpu.roll(found, lanes - k * shard, 1)
            for r in range(count):
                out[r * (lanes // shard) + k, :, count * lanes :] = jnp.where(lane < shard, rolled[r : r + 1], tail)
        for g in range(count):
            for d in range(members):
                out[d, :, g * lanes : (g + 1) * lanes] = values[g]


def near_logits(place, pieces, head, other):
    shard, part = pieces[0].shape[-2:]
    count, width = head.shape
    steps = 2 * count // VOCAB_CHUNK
    size = RING * RING * shard
    hbm = pl.BlockSpec(memory_space=pltpu.HBM)
    block = (RING, RING, RING, shard, VOCAB_CHUNK)
    flops = 2 * 9 * size * part * 2 * count
    return pl.pallas_call(
        near_kernel,
        grid=(steps,),
        in_specs=[pl.BlockSpec(memory_space=pltpu.SMEM)] + [hbm] * 11,
        out_specs=pl.BlockSpec(block, lambda v: (0, 0, 0, 0, v)),
        out_shape=jax.ShapeDtypeStruct(block[:-1] + (2 * count,), jnp.float32),
        scratch_shapes=[
            pltpu.VMEM((3, 3 * size, part), jnp.bfloat16),
            pltpu.VMEM((2, VOCAB_CHUNK, width), jnp.bfloat16),
            pltpu.SemaphoreType.DMA((9,)),
            pltpu.SemaphoreType.DMA((2,)),
        ],
        compiler_params=pltpu.CompilerParams(vmem_limit_bytes=40 * 1024 * 1024),
        cost_estimate=pl.CostEstimate(flops=flops, bytes_accessed=32 << 20, transcendentals=0),
        name="near_logits",
    )(place, *[p.reshape(size, part) for p in pieces], head, other)


def far_losses(place, pieces, near, head, other, sums, pipe_of):
    shard, part = pieces[0].shape[-2:]
    count, width = head.shape
    steps = 2 * count // VOCAB_CHUNK
    size = RING * RING * shard
    tokens = RING * size
    hbm = pl.BlockSpec(memory_space=pltpu.HBM)
    grid = (RING, RING, RING, shard)
    return pl.pallas_call(
        far_kernel,
        grid=(steps,),
        in_specs=[pl.BlockSpec(memory_space=pltpu.SMEM)]
        + [hbm] * 8
        + [
            pl.BlockSpec(grid + (VOCAB_CHUNK,), lambda v: (0, 0, 0, 0, v)),
            pl.BlockSpec(pipe_of.shape, lambda v: (0, 0)),
        ],
        out_specs=pl.BlockSpec((RING**3, 1, tokens + 128), lambda v: (0, 0, 0)),
        out_shape=jax.ShapeDtypeStruct((RING**3, 1, tokens + 128), jnp.float32),
        scratch_shapes=[
            pltpu.VMEM((3, size, part), jnp.bfloat16),
            pltpu.VMEM((2, VOCAB_CHUNK, width), jnp.bfloat16),
            pltpu.VMEM((RING, size, EXTRA), jnp.bfloat16),
            pltpu.VMEM(grid + (128,), jnp.int32),
            pltpu.VMEM(grid + (VOCAB_CHUNK,), jnp.float32),
            pltpu.VMEM(grid + (128,), jnp.float32),
            pltpu.VMEM(grid + (128,), jnp.float32),
            pltpu.VMEM(grid + (128,), jnp.float32),
            pltpu.SemaphoreType.DMA((3,)),
            pltpu.SemaphoreType.DMA((RING,)),
            pltpu.SemaphoreType.DMA((2,)),
        ],
        compiler_params=pltpu.CompilerParams(vmem_limit_bytes=40 * 1024 * 1024),
        name="far_losses",
    )(place, *[p.reshape(size, part) for p in (*pieces, *near)], head, other, sums, pipe_of)


def finish_kernel(mine, stats, pipe_of, losses, pipes):
    lanes = losses.shape[1]
    tokens = pipe_of.shape[1]
    local = stats[:, :, :tokens]
    top = jnp.max(local, axis=0)
    total = top + jnp.log(jnp.sum(jnp.exp(local - top[None]), axis=0))
    tail = jnp.sum(stats[:, :, tokens:], axis=0)
    own = jnp.zeros((1, lanes), jnp.float32)
    for g in range(tokens // lanes):
        own = jnp.where(mine[0] == g, total[:, g * lanes : (g + 1) * lanes], own)
    losses[...] = pltpu.roll(own, mine[1], 1) - tail
    lane = lax.broadcasted_iota(jnp.int32, (1, lanes), 1)
    sums = []
    for k, part in enumerate(split(total)):
        row = jnp.zeros((1, lanes), jnp.float32)
        for p in range(PIPES):
            value = jnp.sum(jnp.where(pipe_of[...] == p, part, 0.0), keepdims=True)
            row = jnp.where(lane == p, value, row)
        sums.append(row - pltpu.roll(tail, lanes - mine[2] - k * PIPES, 1))
    pipes[...] = sums[0] + sums[1]


def finish(mine, stats, pipe_of):
    vmem = pl.BlockSpec(memory_space=pltpu.VMEM)
    return pl.pallas_call(
        finish_kernel,
        in_specs=[pl.BlockSpec(memory_space=pltpu.SMEM), vmem, vmem],
        out_specs=[vmem, vmem],
        out_shape=[jax.ShapeDtypeStruct((1, 128), jnp.float32)] * 2,
        name="finish",
    )(mine, stats, pipe_of)


def shards(hidden, norm_gain, head, targets, route):
    rows = hidden.shape[0]
    x, core, z, y = (lax.axis_index(a) for a in ALL)
    devices = lax.axis_size(ALL)
    pipes = lax.axis_size((X, CORE))
    count = head.shape[0]
    other = lax.ppermute(head, CORE, [(0, 1), (1, 0)])
    near, far = gather(normalize(hidden, norm_gain, targets))
    own = lax.axis_index(ALL)
    partner = ((x * 2 + 1 - core) * RING + z) * RING + y
    at = [sender(axis, offset) for axis in (X, Z, Y) for offset in OFFSETS]
    place = jnp.stack([*at, own * count, partner * count]).astype(jnp.int32)
    sums = near_logits(place, sum(near, []), head, other)
    members = lax.axis_size(CLASS)
    lanes = 128
    pipe_of = lax.dynamic_index_in_dim(route.reshape(RING, 2, RING * RING), core, 1, keepdims=False)
    pipe_of = jnp.repeat(pipe_of.reshape(members), rows).reshape(members * rows // lanes, lanes)
    stats = far_losses(place, far, near[2], head, other, sums, pipe_of)
    stats = lax.all_to_all(stats, CLASS, 0, 0, tiled=True)
    first = lax.axis_index(CLASS) * rows
    mine = jnp.stack([first // lanes, (lanes - first % lanes) % lanes, rows]).astype(jnp.int32)
    losses, sums = finish(mine, stats, pipe_of.reshape(1, members * rows))
    sums = (sums + lax.ppermute(sums, CORE, [(0, 1), (1, 0)])) / (rows * devices // pipes)
    return (losses[0, :rows], sums[0, :pipes])


def solution(mesh):
    torus = Mesh(mesh.devices.reshape(RING, 2, RING, RING), ALL)
    return jax.shard_map(
        shards,
        mesh=torus,
        in_specs=(P(ALL, None), P(), P(ALL, None), P(ALL), P()),
        out_specs=(P(ALL), P()),
        check_vma=False,
    )
```

```python
import functools

import jax
import jax.numpy as jnp
from jax import lax
from jax.experimental import pallas as pl
from jax.experimental.pallas import tpu as pltpu
from jax.sharding import Mesh
from jax.sharding import PartitionSpec as P


X, CORE, Z, Y = "dp_0", "dp_1", "pp_0", "pp_1"
ALL = (X, CORE, Z, Y)
CLASS = (X, Z, Y)
RING = 4
OFFSETS = (0, -1, 1, 2)
ORDERS = ((Y, Z, X), (X, Y, Z), (Z, X, Y))
EXTRA = 128
VOCAB_CHUNK = 512


def shift(x, axis, offset):
    pairs = []
    for i in range(RING):
        for core in range(2):
            to = (i - offset * (1 - 2 * core)) % RING
            pairs.append((i * 2 + core, to * 2 + core) if axis == X else (core * RING + i, core * RING + to))
    return lax.ppermute(x, (X, CORE) if axis == X else (CORE, axis), pairs)


def sender(axis, offset):
    return (lax.axis_index(axis) + offset * (1 - 2 * lax.axis_index(CORE))) % RING


def norm_kernel(targets, hidden, gain, *parts):
    rows, width = hidden.shape
    wide = hidden[...].astype(jnp.float32)
    factor = lax.rsqrt(jnp.mean(wide * wide, axis=1, keepdims=True) + 1e-05)
    normed = (wide * factor * gain[...]).astype(jnp.bfloat16)
    row = lax.broadcasted_iota(jnp.int32, (rows, EXTRA), 0)
    lane = lax.broadcasted_iota(jnp.int32, (rows, EXTRA), 1)
    ids = jnp.zeros((rows, EXTRA), jnp.int32)
    for i in range(rows):
        ids = jnp.where(row == i, targets[i], ids)
    digit = jnp.where(lane == 0, ids >> 16, jnp.where(lane == 1, (ids >> 8) & 255, ids & 255))
    digit = jnp.where(lane < 3, digit, 0).astype(jnp.float32).astype(jnp.bfloat16)
    part = (width + EXTRA) // 3
    parts[0][...] = normed[:, :part]
    parts[1][...] = normed[:, part : 2 * part]
    parts[2][:, : part - EXTRA] = normed[:, 2 * part :]
    parts[2][:, part - EXTRA :] = digit


def normalize(hidden, gain, targets):
    rows, width = hidden.shape
    part = (width + EXTRA) // 3
    vmem = pl.BlockSpec(memory_space=pltpu.VMEM)
    return pl.pallas_call(
        norm_kernel,
        in_specs=[pl.BlockSpec(memory_space=pltpu.SMEM), vmem, vmem],
        out_specs=[vmem] * 3,
        out_shape=[jax.ShapeDtypeStruct((rows, part), jnp.bfloat16)] * 3,
        name="normalize",
    )(targets, hidden, gain.reshape(1, width))


def gather(parts):
    for phase in range(2):
        parts = [
            jnp.stack([x] + [shift(x, order[phase], offset) for offset in OFFSETS[1:]])
            for x, order in zip(parts, ORDERS)
        ]
    near = [[x] + [shift(x, order[2], offset) for offset in OFFSETS[1:3]] for x, order in zip(parts, ORDERS)]
    far = [shift(n[1], order[2], OFFSETS[1]) for n, order in zip(near, ORDERS)]
    return near, far


PIPES = 8


def split(x):
    coarse = jnp.floor(x * (1.0 / 256.0)) * 256.0
    return coarse, x - coarse


CONTRACT = (((1,), (1,)), ((), ()))
NEAR = RING - 1


def head_copies(heads, vocab, sems):
    per_head = heads[0].shape[0] // VOCAB_CHUNK
    for c in range(2 * per_head):
        src = heads[c // per_head].at[pl.ds((c % per_head) * VOCAB_CHUNK, VOCAB_CHUNK)]
        yield pltpu.make_async_copy(src, vocab.at[c], sems.at[c])


def statistics(place, tokens, vocab, copies):
    width = vocab.shape[-1]
    lanes = EXTRA
    weight = lax.broadcasted_iota(jnp.int32, (EXTRA, lanes), 0)
    weight = jnp.where(weight == 0, 65536, jnp.where(weight == 1, 256, jnp.where(weight == 2, 1, 0)))
    weight = weight.astype(jnp.float32).astype(jnp.bfloat16)
    labels = jnp.dot(tokens[:, width:], weight, preferred_element_type=jnp.float32).astype(jnp.int32)
    tokens = tokens[:, :width]
    lane = lax.broadcasted_iota(jnp.int32, labels.shape, 1)
    peak = jnp.full(labels.shape, -jnp.inf, jnp.float32)
    mass = jnp.zeros(labels.shape, jnp.float32)
    hit = jnp.zeros(labels.shape, jnp.float32)
    per_head = len(copies) // 2
    for c, copy in enumerate(copies):
        copy.wait()
        logits = lax.dot_general(tokens, vocab[c], CONTRACT, preferred_element_type=jnp.float32)
        label = labels - (place[12 + c // per_head] + (c % per_head) * VOCAB_CHUNK)
        parts = [logits[:, i * lanes : (i + 1) * lanes] for i in range(VOCAB_CHUNK // lanes)]
        top = functools.reduce(jnp.maximum, parts, peak)
        mass = mass * jnp.exp(peak - top)
        for i, value in enumerate(parts):
            mass += jnp.exp(value - top)
            hit += jnp.where(label == lane + i * lanes, value, 0.0)
        peak = top
    top = jnp.max(peak, axis=1, keepdims=True)
    value = top + jnp.log(jnp.sum(mass * jnp.exp(peak - top), axis=1, keepdims=True))
    return value, jnp.sum(hit, axis=1, keepdims=True)


def near_kernel(place, *refs):
    a, b, c, heads, out, rows, vocab, row_sem, head_sems = (
        refs[:3], refs[3:6], refs[6:9], refs[9:11], *refs[11:],
    )
    part = a[0].shape[-1]
    near = pl.ds(0, NEAR)
    pairs = []
    for i in range(NEAR):
        pairs.append((a[i].at[near, near], rows.at[i, :, :, :, pl.ds(0, part)]))
        pairs.append((c[i].at[near, near], rows.at[:, :, i, :, pl.ds(2 * part, part)]))
        for x in range(NEAR):
            pairs.append((b[i].at[near, x], rows.at[x, i, :, :, pl.ds(part, part)]))
    for src, dst in pairs:
        pltpu.make_async_copy(src, dst, row_sem).start()
    copies = list(head_copies(heads, vocab, head_sems))
    for copy in copies:
        copy.start()
    pltpu.make_async_copy(rows, rows, row_sem).wait()
    count = out.shape[1]
    tokens = rows[...].reshape(count, 3 * part)
    for k, column in enumerate(statistics(place, tokens, vocab, copies)):
        out[k] = jnp.broadcast_to(column, out.shape[1:])


def far_kernel(place, *refs):
    a, b, c, heads, near_stats, pipe_of, out = refs[:4], refs[4:8], refs[8:12], refs[12:14], *refs[14:17]
    groups, rows, vocab, values_at, hits_at, row_sems, head_sems = refs[17:20], *refs[20:]
    part = a[0].shape[-1]
    shard = a[0].shape[-2]
    near, last = pl.ds(0, NEAR), RING - 1
    low, mid, high = pl.ds(0, part), pl.ds(part, part), pl.ds(2 * part, part)
    by_x, by_z, by_y = groups
    pairs = [(0, a[last], by_x.at[:, :, :, low]), (2, c[last].at[near, near], by_y.at[:, :, :, high])]
    for i in range(RING):
        pairs.append((0, b[i].at[:, last], by_x.at[i, :, :, mid]))
        pairs.append((0, c[i].at[last], by_x.at[:, i, :, high]))
        pairs.append((1, c[i].at[near, last], by_z.at[:, i, :, high]))
    for i in range(NEAR):
        pairs.append((1, a[i].at[last], by_z.at[i, :, :, low]))
        pairs.append((1, b[last].at[:, i], by_z.at[i, :, :, mid]))
        pairs.append((2, a[i].at[near, last], by_y.at[i, :, :, low]))
        pairs.append((2, b[i].at[last, near], by_y.at[:, i, :, mid]))
    for g, src, dst in pairs:
        pltpu.make_async_copy(src, dst, row_sems.at[g]).start()
    copies = list(head_copies(heads, vocab, head_sems))
    for copy in copies:
        copy.start()
    start = 0
    for g, group in enumerate(groups):
        size = group.shape[0] * group.shape[1] * shard
        pltpu.make_async_copy(group, group, row_sems.at[g]).wait()
        rows[pl.ds(start, size)] = group[...].reshape(size, 3 * part)
        start += size
    lanes = EXTRA
    far = [(last, z, y) for z in range(RING) for y in range(RING)]
    far += [(x, last, y) for x in range(NEAR) for y in range(RING)]
    far += [(x, z, last) for x in range(NEAR) for z in range(NEAR)]
    close = [(x, z, y) for x in range(NEAR) for z in range(NEAR) for y in range(NEAR)]

    def member(x, z, y):
        return (place[x] * RING + place[RING + z]) * RING + place[2 * RING + y]

    for k, column in enumerate(statistics(place, rows[...], vocab, copies)):
        to = (values_at, hits_at)[k]
        for s, spot in enumerate(far):
            to[member(*spot)] = jnp.broadcast_to(column[s * shard : (s + 1) * shard], (shard, lanes))
        for s, spot in enumerate(close):
            to[member(*spot)] = near_stats[k, s * shard : (s + 1) * shard]

    row = lax.broadcasted_iota(jnp.int32, (lanes, lanes), 0)
    diagonal = row == lax.broadcasted_iota(jnp.int32, (lanes, lanes), 1)
    count = pipe_of.shape[0]
    per = lanes // shard

    def lines(columns):
        square = [columns[g * per : (g + 1) * per].reshape(lanes, lanes) for g in range(count)]
        return [jnp.sum(jnp.where(diagonal, s, 0.0), axis=0, keepdims=True) for s in square]

    values = lines(values_at)
    found = jnp.concatenate(lines(hits_at), axis=0)
    coarse, fine = split(found)
    lane = lax.broadcasted_iota(jnp.int32, (1, lanes), 1)
    tail = jnp.zeros((1, lanes), jnp.float32)
    for p in range(PIPES):
        mine = pipe_of[...] == p
        for k, term in enumerate((coarse, fine)):
            value = jnp.sum(jnp.where(mine, term, 0.0), keepdims=True)
            tail = jnp.where(lane == shard + k * PIPES + p, value, tail)
    for k in range(per):
        rolled = found if k == 0 else pltpu.roll(found, lanes - k * shard, 1)
        for r in range(count):
            out[r * per + k, :, count * lanes :] = jnp.where(lane < shard, rolled[r : r + 1], tail)
    for g in range(count):
        for d in range(out.shape[0]):
            out[d, :, g * lanes : (g + 1) * lanes] = values[g]


def near_losses(place, near, head, other):
    shard, part = near[0][0].shape[-2:]
    count, width = head.shape
    chunks = 2 * count // VOCAB_CHUNK
    tokens = NEAR**3 * shard
    hbm = pl.BlockSpec(memory_space=pltpu.HBM)
    return pl.pallas_call(
        near_kernel,
        in_specs=[pl.BlockSpec(memory_space=pltpu.SMEM)] + [hbm] * 11,
        out_specs=pl.BlockSpec(memory_space=pltpu.VMEM),
        out_shape=jax.ShapeDtypeStruct((2, tokens, EXTRA), jnp.float32),
        scratch_shapes=[
            pltpu.VMEM((NEAR, NEAR, NEAR, shard, 3 * part), jnp.bfloat16),
            pltpu.VMEM((chunks, VOCAB_CHUNK, width), jnp.bfloat16),
            pltpu.SemaphoreType.DMA(()),
            pltpu.SemaphoreType.DMA((chunks,)),
        ],
        compiler_params=pltpu.CompilerParams(vmem_limit_bytes=40 * 1024 * 1024),
        cost_estimate=pl.CostEstimate(
            flops=4 * tokens * width * count, bytes_accessed=20 << 20, transcendentals=2 * tokens * count
        ),
        name="near_losses",
    )(place, *sum(near, []), head, other)


def far_losses(place, near, far, head, other, near_stats, pipe_of):
    shard, part = near[0][0].shape[-2:]
    count, width = head.shape
    chunks = 2 * count // VOCAB_CHUNK
    members = RING**3
    tokens = members * shard
    hbm = pl.BlockSpec(memory_space=pltpu.HBM)
    vmem = pl.BlockSpec(memory_space=pltpu.VMEM)
    groups = ((RING, RING), (NEAR, RING), (NEAR, NEAR))
    return pl.pallas_call(
        far_kernel,
        in_specs=[pl.BlockSpec(memory_space=pltpu.SMEM)] + [hbm] * 14 + [vmem] * 2,
        out_specs=vmem,
        out_shape=jax.ShapeDtypeStruct((members, 1, tokens + EXTRA), jnp.float32),
        scratch_shapes=[pltpu.VMEM(g + (shard, 3 * part), jnp.bfloat16) for g in groups]
        + [
            pltpu.VMEM((tokens - NEAR**3 * shard, 3 * part), jnp.bfloat16),
            pltpu.VMEM((chunks, VOCAB_CHUNK, width), jnp.bfloat16),
            pltpu.VMEM((members, shard, EXTRA), jnp.float32),
            pltpu.VMEM((members, shard, EXTRA), jnp.float32),
            pltpu.SemaphoreType.DMA((3,)),
            pltpu.SemaphoreType.DMA((chunks,)),
        ],
        compiler_params=pltpu.CompilerParams(vmem_limit_bytes=48 * 1024 * 1024),
        name="far_losses",
    )(place, *sum(([*n, f] for n, f in zip(near, far)), []), head, other, near_stats, pipe_of)


def finish_kernel(mine, stats, pipe_of, losses, pipes):
    lanes = losses.shape[1]
    tokens = pipe_of.shape[1]
    local = stats[:, :, :tokens]
    top = jnp.max(local, axis=0)
    total = top + jnp.log(jnp.sum(jnp.exp(local - top[None]), axis=0))
    tail = jnp.sum(stats[:, :, tokens:], axis=0)
    own = jnp.zeros((1, lanes), jnp.float32)
    for g in range(tokens // lanes):
        own = jnp.where(mine[0] == g, total[:, g * lanes : (g + 1) * lanes], own)
    losses[...] = pltpu.roll(own, mine[1], 1) - tail
    lane = lax.broadcasted_iota(jnp.int32, (1, lanes), 1)
    sums = []
    for k, part in enumerate(split(total)):
        row = jnp.zeros((1, lanes), jnp.float32)
        for p in range(PIPES):
            value = jnp.sum(jnp.where(pipe_of[...] == p, part, 0.0), keepdims=True)
            row = jnp.where(lane == p, value, row)
        sums.append(row - pltpu.roll(tail, lanes - mine[2] - k * PIPES, 1))
    pipes[...] = sums[0] + sums[1]


def finish(mine, stats, pipe_of):
    vmem = pl.BlockSpec(memory_space=pltpu.VMEM)
    return pl.pallas_call(
        finish_kernel,
        in_specs=[pl.BlockSpec(memory_space=pltpu.SMEM), vmem, vmem],
        out_specs=[vmem, vmem],
        out_shape=[jax.ShapeDtypeStruct((1, 128), jnp.float32)] * 2,
        name="finish",
    )(mine, stats, pipe_of)


def shards(hidden, norm_gain, head, targets, route):
    rows = hidden.shape[0]
    x, core, z, y = (lax.axis_index(a) for a in ALL)
    devices = lax.axis_size(ALL)
    pipes = lax.axis_size((X, CORE))
    count = head.shape[0]
    other = lax.ppermute(head, CORE, [(0, 1), (1, 0)])
    near, far = gather(normalize(hidden, norm_gain, targets))
    own = lax.axis_index(ALL)
    partner = ((x * 2 + 1 - core) * RING + z) * RING + y
    at = [sender(axis, offset) for axis in (X, Z, Y) for offset in OFFSETS]
    place = jnp.stack([*at, own * count, partner * count]).astype(jnp.int32)
    near_stats = near_losses(place, near, head, other)
    members = lax.axis_size(CLASS)
    lanes = 128
    pipe_of = lax.dynamic_index_in_dim(route.reshape(RING, 2, RING * RING), core, 1, keepdims=False)
    pipe_of = jnp.repeat(pipe_of.reshape(members), rows).reshape(members * rows // lanes, lanes)
    stats = far_losses(place, near, far, head, other, near_stats, pipe_of)
    stats = lax.all_to_all(stats, CLASS, 0, 0, tiled=True)
    first = lax.axis_index(CLASS) * rows
    mine = jnp.stack([first // lanes, (lanes - first % lanes) % lanes, rows]).astype(jnp.int32)
    losses, sums = finish(mine, stats, pipe_of.reshape(1, members * rows))
    sums = (sums + lax.ppermute(sums, CORE, [(0, 1), (1, 0)])) / (rows * devices // pipes)
    return (losses[0, :rows], sums[0, :pipes])


def solution(mesh):
    torus = Mesh(mesh.devices.reshape(RING, 2, RING, RING), ALL)
    return jax.shard_map(
        shards,
        mesh=torus,
        in_specs=(P(ALL, None), P(), P(ALL, None), P(ALL), P()),
        out_specs=(P(ALL), P()),
        check_vma=False,
    )
```

```python
import functools

import jax
import jax.numpy as jnp
from jax import lax
from jax.experimental import pallas as pl
from jax.experimental.pallas import tpu as pltpu
from jax.sharding import Mesh
from jax.sharding import PartitionSpec as P


X, CORE, Z, Y = "dp_0", "dp_1", "pp_0", "pp_1"
ALL = (X, CORE, Z, Y)
CLASS = (X, Z, Y)
RING = 4
OFFSETS = (0, -1, 1, 2)
ORDERS = ((Y, Z, X), (Y, X, Z), (Z, X, Y))
EXTRA = 128
VOCAB_CHUNK = 512


def shift(x, axis, offset):
    pairs = []
    for i in range(RING):
        for core in range(2):
            to = (i - offset * (1 - 2 * core)) % RING
            pairs.append((i * 2 + core, to * 2 + core) if axis == X else (core * RING + i, core * RING + to))
    return lax.ppermute(x, (X, CORE) if axis == X else (CORE, axis), pairs)


def sender(axis, offset):
    return (lax.axis_index(axis) + offset * (1 - 2 * lax.axis_index(CORE))) % RING


def norm_kernel(targets, hidden, gain, *parts):
    rows, width = hidden.shape
    wide = hidden[...].astype(jnp.float32)
    factor = lax.rsqrt(jnp.mean(wide * wide, axis=1, keepdims=True) + 1e-05)
    normed = (wide * factor * gain[...]).astype(jnp.bfloat16)
    row = lax.broadcasted_iota(jnp.int32, (rows, EXTRA), 0)
    lane = lax.broadcasted_iota(jnp.int32, (rows, EXTRA), 1)
    ids = jnp.zeros((rows, EXTRA), jnp.int32)
    for i in range(rows):
        ids = jnp.where(row == i, targets[i], ids)
    digit = jnp.where(lane == 0, ids >> 16, jnp.where(lane == 1, (ids >> 8) & 255, ids & 255))
    digit = jnp.where(lane < 3, digit, 0).astype(jnp.float32).astype(jnp.bfloat16)
    part = (width + EXTRA) // 3
    parts[0][...] = normed[:, : 2 * part]
    parts[1][:, : part - EXTRA] = normed[:, 2 * part :]
    parts[1][:, part - EXTRA :] = digit


def normalize(hidden, gain, targets):
    rows, width = hidden.shape
    part = (width + EXTRA) // 3
    vmem = pl.BlockSpec(memory_space=pltpu.VMEM)
    return pl.pallas_call(
        norm_kernel,
        in_specs=[pl.BlockSpec(memory_space=pltpu.SMEM), vmem, vmem],
        out_specs=[vmem] * 2,
        out_shape=[jax.ShapeDtypeStruct((rows, 2 * part), jnp.bfloat16), jax.ShapeDtypeStruct((rows, part), jnp.bfloat16)],
        name="normalize",
    )(targets, hidden, gain.reshape(1, width))


def ring(x, axis):
    return [x] + [shift(x, axis, offset) for offset in OFFSETS[1:]]


def gather(both, third):
    part = third.shape[1]
    both = ring(both, ORDERS[0][0])
    third = ring(third, ORDERS[2][0])
    parts = [
        jnp.stack([x[:, :part] for x in both]),
        jnp.stack([x[:, part:] for x in both]),
        jnp.stack(third),
    ]
    parts = [jnp.stack(ring(x, order[1])) for x, order in zip(parts, ORDERS)]
    near = [[x] + [shift(x, order[2], offset) for offset in OFFSETS[1:3]] for x, order in zip(parts, ORDERS)]
    far = [shift(n[1], order[2], OFFSETS[1]) for n, order in zip(near, ORDERS)]
    return near, far


PIPES = 8


def split(x):
    coarse = jnp.floor(x * (1.0 / 256.0)) * 256.0
    return coarse, x - coarse


CONTRACT = (((1,), (1,)), ((), ()))
NEAR = RING - 1


def chunks_of(count):
    half = VOCAB_CHUNK // 2
    first = [(0, 0, half), (0, half, half)]
    return first + [(k, s, VOCAB_CHUNK) for k in range(2) for s in range(0, count, VOCAB_CHUNK) if k or s]


def head_copies(heads, vocab, sems):
    count = heads[0].shape[0]
    for c, (k, start, size) in enumerate(chunks_of(count)):
        src = heads[k].at[pl.ds(start, size)]
        yield pltpu.make_async_copy(src, vocab.at[pl.ds(k * count + start, size)], sems.at[c])


def statistics(place, tokens, vocab, copies):
    width = vocab.shape[-1]
    lanes = EXTRA
    weight = lax.broadcasted_iota(jnp.int32, (EXTRA, lanes), 0)
    weight = jnp.where(weight == 0, 65536, jnp.where(weight == 1, 256, jnp.where(weight == 2, 1, 0)))
    weight = weight.astype(jnp.float32).astype(jnp.bfloat16)
    labels = jnp.dot(tokens[:, width:], weight, preferred_element_type=jnp.float32).astype(jnp.int32)
    tokens = tokens[:, :width]
    lane = lax.broadcasted_iota(jnp.int32, labels.shape, 1)
    peak = jnp.full(labels.shape, -jnp.inf, jnp.float32)
    mass = jnp.zeros(labels.shape, jnp.float32)
    hit = jnp.zeros(labels.shape, jnp.float32)
    count = vocab.shape[0] // 2
    for copy, (k, start, size) in zip(copies, chunks_of(count)):
        copy.wait()
        words = vocab[pl.ds(k * count + start, size)]
        logits = lax.dot_general(tokens, words, CONTRACT, preferred_element_type=jnp.float32)
        label = labels - (place[12 + k] + start)
        parts = [logits[:, i * lanes : (i + 1) * lanes] for i in range(size // lanes)]
        top = functools.reduce(jnp.maximum, parts, peak)
        mass = mass * jnp.exp(peak - top)
        for i, value in enumerate(parts):
            mass += jnp.exp(value - top)
            hit += jnp.where(label == lane + i * lanes, value, 0.0)
        peak = top
    top = jnp.max(peak, axis=1, keepdims=True)
    value = top + jnp.log(jnp.sum(mass * jnp.exp(peak - top), axis=1, keepdims=True))
    return value, jnp.sum(hit, axis=1, keepdims=True)


def near_kernel(place, *refs):
    a, b, c, heads, out, rows, vocab, row_sem, head_sems = (
        refs[:3], refs[3:6], refs[6:9], refs[9:11], *refs[11:],
    )
    part = a[0].shape[-1]
    near = pl.ds(0, NEAR)
    pairs = []
    for i in range(NEAR):
        pairs.append((a[i].at[near, near], rows.at[i, :, :, :, pl.ds(0, part)]))
        pairs.append((c[i].at[near, near], rows.at[:, :, i, :, pl.ds(2 * part, part)]))
        pairs.append((b[i].at[near, near], rows.at[:, i, :, :, pl.ds(part, part)]))
    for src, dst in pairs:
        pltpu.make_async_copy(src, dst, row_sem).start()
    copies = list(head_copies(heads, vocab, head_sems))
    for copy in copies:
        copy.start()
    pltpu.make_async_copy(rows, rows, row_sem).wait()
    count = out.shape[1]
    tokens = rows[...].reshape(count, 3 * part)
    for k, column in enumerate(statistics(place, tokens, vocab, copies)):
        out[k] = jnp.broadcast_to(column, out.shape[1:])


def far_kernel(place, *refs):
    a, b, c, heads, near_stats, pipe_of, out = refs[:4], refs[4:8], refs[8:12], refs[12:14], *refs[14:17]
    groups, rows, vocab, values_at, hits_at, row_sems, head_sems = refs[17:20], *refs[20:]
    part = a[0].shape[-1]
    shard = a[0].shape[-2]
    near, last = pl.ds(0, NEAR), RING - 1
    low, mid, high = pl.ds(0, part), pl.ds(part, part), pl.ds(2 * part, part)
    by_x, by_z, by_y = groups
    pairs = [(0, a[last], by_x.at[:, :, :, low]), (1, b[last].at[near], by_z.at[:, :, :, mid])]
    pairs += [(2, c[last].at[near, near], by_y.at[:, :, :, high])]
    for i in range(RING):
        pairs.append((0, b[i].at[last], by_x.at[i, :, :, mid]))
        pairs.append((0, c[i].at[last], by_x.at[:, i, :, high]))
        pairs.append((1, c[i].at[near, last], by_z.at[:, i, :, high]))
    for i in range(NEAR):
        pairs.append((1, a[i].at[last], by_z.at[i, :, :, low]))
        pairs.append((2, a[i].at[near, last], by_y.at[i, :, :, low]))
        pairs.append((2, b[i].at[near, last], by_y.at[:, i, :, mid]))
    for g, src, dst in pairs:
        pltpu.make_async_copy(src, dst, row_sems.at[g]).start()
    copies = list(head_copies(heads, vocab, head_sems))
    for copy in copies:
        copy.start()
    start = 0
    for g, group in enumerate(groups):
        size = group.shape[0] * group.shape[1] * shard
        pltpu.make_async_copy(group, group, row_sems.at[g]).wait()
        rows[pl.ds(start, size)] = group[...].reshape(size, 3 * part)
        start += size
    lanes = EXTRA
    far = [(last, z, y) for z in range(RING) for y in range(RING)]
    far += [(x, last, y) for x in range(NEAR) for y in range(RING)]
    far += [(x, z, last) for x in range(NEAR) for z in range(NEAR)]
    close = [(x, z, y) for x in range(NEAR) for z in range(NEAR) for y in range(NEAR)]

    def member(x, z, y):
        return (place[x] * RING + place[RING + z]) * RING + place[2 * RING + y]

    for k, column in enumerate(statistics(place, rows[...], vocab, copies)):
        to = (values_at, hits_at)[k]
        for s, spot in enumerate(far):
            to[member(*spot)] = jnp.broadcast_to(column[s * shard : (s + 1) * shard], (shard, lanes))
        for s, spot in enumerate(close):
            to[member(*spot)] = near_stats[k, s * shard : (s + 1) * shard]

    row = lax.broadcasted_iota(jnp.int32, (lanes, lanes), 0)
    diagonal = row == lax.broadcasted_iota(jnp.int32, (lanes, lanes), 1)
    count = pipe_of.shape[0]
    per = lanes // shard

    def lines(columns):
        square = [columns[g * per : (g + 1) * per].reshape(lanes, lanes) for g in range(count)]
        return [jnp.sum(jnp.where(diagonal, s, 0.0), axis=0, keepdims=True) for s in square]

    values = lines(values_at)
    found = jnp.concatenate(lines(hits_at), axis=0)
    coarse, fine = split(found)
    lane = lax.broadcasted_iota(jnp.int32, (1, lanes), 1)
    tail = jnp.zeros((1, lanes), jnp.float32)
    for p in range(PIPES):
        mine = pipe_of[...] == p
        for k, term in enumerate((coarse, fine)):
            value = jnp.sum(jnp.where(mine, term, 0.0), keepdims=True)
            tail = jnp.where(lane == shard + k * PIPES + p, value, tail)
    for k in range(per):
        rolled = found if k == 0 else pltpu.roll(found, lanes - k * shard, 1)
        for r in range(count):
            out[r * per + k, :, count * lanes :] = jnp.where(lane < shard, rolled[r : r + 1], tail)
    for g in range(count):
        for d in range(out.shape[0]):
            out[d, :, g * lanes : (g + 1) * lanes] = values[g]


def near_losses(place, near, head, other):
    shard, part = near[0][0].shape[-2:]
    count, width = head.shape
    chunks = len(chunks_of(count))
    tokens = NEAR**3 * shard
    hbm = pl.BlockSpec(memory_space=pltpu.HBM)
    return pl.pallas_call(
        near_kernel,
        in_specs=[pl.BlockSpec(memory_space=pltpu.SMEM)] + [hbm] * 11,
        out_specs=pl.BlockSpec(memory_space=pltpu.VMEM),
        out_shape=jax.ShapeDtypeStruct((2, tokens, EXTRA), jnp.float32),
        scratch_shapes=[
            pltpu.VMEM((NEAR, NEAR, NEAR, shard, 3 * part), jnp.bfloat16),
            pltpu.VMEM((2 * count, width), jnp.bfloat16),
            pltpu.SemaphoreType.DMA(()),
            pltpu.SemaphoreType.DMA((chunks,)),
        ],
        compiler_params=pltpu.CompilerParams(vmem_limit_bytes=40 * 1024 * 1024),
        cost_estimate=pl.CostEstimate(
            flops=4 * tokens * width * count, bytes_accessed=20 << 20, transcendentals=2 * tokens * count
        ),
        name="near_losses",
    )(place, *sum(near, []), head, other)


def far_losses(place, near, far, head, other, near_stats, pipe_of):
    shard, part = near[0][0].shape[-2:]
    count, width = head.shape
    chunks = len(chunks_of(count))
    members = RING**3
    tokens = members * shard
    hbm = pl.BlockSpec(memory_space=pltpu.HBM)
    vmem = pl.BlockSpec(memory_space=pltpu.VMEM)
    groups = ((RING, RING), (NEAR, RING), (NEAR, NEAR))
    return pl.pallas_call(
        far_kernel,
        in_specs=[pl.BlockSpec(memory_space=pltpu.SMEM)] + [hbm] * 14 + [vmem] * 2,
        out_specs=vmem,
        out_shape=jax.ShapeDtypeStruct((members, 1, tokens + EXTRA), jnp.float32),
        scratch_shapes=[pltpu.VMEM(g + (shard, 3 * part), jnp.bfloat16) for g in groups]
        + [
            pltpu.VMEM((tokens - NEAR**3 * shard, 3 * part), jnp.bfloat16),
            pltpu.VMEM((2 * count, width), jnp.bfloat16),
            pltpu.VMEM((members, shard, EXTRA), jnp.float32),
            pltpu.VMEM((members, shard, EXTRA), jnp.float32),
            pltpu.SemaphoreType.DMA((3,)),
            pltpu.SemaphoreType.DMA((chunks,)),
        ],
        compiler_params=pltpu.CompilerParams(vmem_limit_bytes=48 * 1024 * 1024),
        name="far_losses",
    )(place, *sum(([*n, f] for n, f in zip(near, far)), []), head, other, near_stats, pipe_of)


def finish_kernel(mine, stats, pipe_of, losses, pipes):
    lanes = losses.shape[1]
    tokens = pipe_of.shape[1]
    local = stats[:, :, :tokens]
    top = jnp.max(local, axis=0)
    total = top + jnp.log(jnp.sum(jnp.exp(local - top[None]), axis=0))
    tail = jnp.sum(stats[:, :, tokens:], axis=0)
    own = jnp.zeros((1, lanes), jnp.float32)
    for g in range(tokens // lanes):
        own = jnp.where(mine[0] == g, total[:, g * lanes : (g + 1) * lanes], own)
    losses[...] = pltpu.roll(own, mine[1], 1) - tail
    lane = lax.broadcasted_iota(jnp.int32, (1, lanes), 1)
    sums = []
    for k, part in enumerate(split(total)):
        row = jnp.zeros((1, lanes), jnp.float32)
        for p in range(PIPES):
            value = jnp.sum(jnp.where(pipe_of[...] == p, part, 0.0), keepdims=True)
            row = jnp.where(lane == p, value, row)
        sums.append(row - pltpu.roll(tail, lanes - mine[2] - k * PIPES, 1))
    pipes[...] = sums[0] + sums[1]


def finish(mine, stats, pipe_of):
    vmem = pl.BlockSpec(memory_space=pltpu.VMEM)
    return pl.pallas_call(
        finish_kernel,
        in_specs=[pl.BlockSpec(memory_space=pltpu.SMEM), vmem, vmem],
        out_specs=[vmem, vmem],
        out_shape=[jax.ShapeDtypeStruct((1, 128), jnp.float32)] * 2,
        name="finish",
    )(mine, stats, pipe_of)


def shards(hidden, norm_gain, head, targets, route):
    rows = hidden.shape[0]
    x, core, z, y = (lax.axis_index(a) for a in ALL)
    devices = lax.axis_size(ALL)
    pipes = lax.axis_size((X, CORE))
    count = head.shape[0]
    other = lax.ppermute(head, CORE, [(0, 1), (1, 0)])
    near, far = gather(*normalize(hidden, norm_gain, targets))
    own = lax.axis_index(ALL)
    partner = ((x * 2 + 1 - core) * RING + z) * RING + y
    at = [sender(axis, offset) for axis in (X, Z, Y) for offset in OFFSETS]
    place = jnp.stack([*at, own * count, partner * count]).astype(jnp.int32)
    near_stats = near_losses(place, near, head, other)
    members = lax.axis_size(CLASS)
    lanes = 128
    pipe_of = lax.dynamic_index_in_dim(route.reshape(RING, 2, RING * RING), core, 1, keepdims=False)
    pipe_of = jnp.repeat(pipe_of.reshape(members), rows).reshape(members * rows // lanes, lanes)
    stats = far_losses(place, near, far, head, other, near_stats, pipe_of)
    stats = lax.all_to_all(stats, CLASS, 0, 0, tiled=True)
    first = lax.axis_index(CLASS) * rows
    mine = jnp.stack([first // lanes, (lanes - first % lanes) % lanes, rows]).astype(jnp.int32)
    losses, sums = finish(mine, stats, pipe_of.reshape(1, members * rows))
    sums = (sums + lax.ppermute(sums, CORE, [(0, 1), (1, 0)])) / (rows * devices // pipes)
    return (losses[0, :rows], sums[0, :pipes])


def solution(mesh):
    torus = Mesh(mesh.devices.reshape(RING, 2, RING, RING), ALL)
    return jax.shard_map(
        shards,
        mesh=torus,
        in_specs=(P(ALL, None), P(), P(ALL, None), P(ALL), P()),
        out_specs=(P(ALL), P()),
        check_vma=False,
    )
```

```python
import functools

import jax
import jax.numpy as jnp
from jax import lax
from jax.experimental import pallas as pl
from jax.experimental.pallas import tpu as pltpu
from jax.sharding import Mesh
from jax.sharding import PartitionSpec as P


X, CORE, Z, Y = "dp_0", "dp_1", "pp_0", "pp_1"
ALL = (X, CORE, Z, Y)
CLASS = (X, Z, Y)
RING = 4
OFFSETS = (0, -1, 1, 2)
ORDERS = ((Y, Z, X), (Y, X, Z), (Z, X, Y))
EXTRA = 128
VOCAB_CHUNK = 512


def shift(x, axis, offset):
    pairs = []
    for i in range(RING):
        for core in range(2):
            to = (i - offset * (1 - 2 * core)) % RING
            pairs.append((i * 2 + core, to * 2 + core) if axis == X else (core * RING + i, core * RING + to))
    return lax.ppermute(x, (X, CORE) if axis == X else (CORE, axis), pairs)


def sender(axis, offset):
    return (lax.axis_index(axis) + offset * (1 - 2 * lax.axis_index(CORE))) % RING


def norm_kernel(targets, hidden, gain, *parts):
    rows, width = hidden.shape
    wide = hidden[...].astype(jnp.float32)
    factor = lax.rsqrt(jnp.mean(wide * wide, axis=1, keepdims=True) + 1e-05)
    normed = (wide * factor * gain[...]).astype(jnp.bfloat16)
    row = lax.broadcasted_iota(jnp.int32, (rows, EXTRA), 0)
    lane = lax.broadcasted_iota(jnp.int32, (rows, EXTRA), 1)
    ids = jnp.zeros((rows, EXTRA), jnp.int32)
    for i in range(rows):
        ids = jnp.where(row == i, targets[i], ids)
    digit = jnp.where(lane == 0, ids >> 16, jnp.where(lane == 1, (ids >> 8) & 255, ids & 255))
    digit = jnp.where(lane < 3, digit, 0).astype(jnp.float32).astype(jnp.bfloat16)
    part = (width + EXTRA) // 3
    parts[0][...] = normed[:, : 2 * part]
    parts[1][:, : part - EXTRA] = normed[:, 2 * part :]
    parts[1][:, part - EXTRA :] = digit


def normalize(hidden, gain, targets):
    rows, width = hidden.shape
    part = (width + EXTRA) // 3
    vmem = pl.BlockSpec(memory_space=pltpu.VMEM)
    return pl.pallas_call(
        norm_kernel,
        in_specs=[pl.BlockSpec(memory_space=pltpu.SMEM), vmem, vmem],
        out_specs=[vmem] * 2,
        out_shape=[jax.ShapeDtypeStruct((rows, 2 * part), jnp.bfloat16), jax.ShapeDtypeStruct((rows, part), jnp.bfloat16)],
        name="normalize",
    )(targets, hidden, gain.reshape(1, width))


def ring(x, axis):
    return [x] + [shift(x, axis, offset) for offset in OFFSETS[1:]]


def gather(both, third):
    part = third.shape[1]
    both = ring(both, ORDERS[0][0])
    third = ring(third, ORDERS[2][0])
    parts = [
        jnp.stack([x[:, :part] for x in both]),
        jnp.stack([x[:, part:] for x in both]),
        jnp.stack(third),
    ]
    parts = [jnp.stack(ring(x, order[1])) for x, order in zip(parts, ORDERS)]
    near = [[x] + [shift(x, order[2], offset) for offset in OFFSETS[1:3]] for x, order in zip(parts, ORDERS)]
    far = [shift(n[1], order[2], OFFSETS[1]) for n, order in zip(near, ORDERS)]
    return near, far


PIPES = 8


def split(x):
    coarse = jnp.floor(x * (1.0 / 256.0)) * 256.0
    return coarse, x - coarse


CONTRACT = (((1,), (1,)), ((), ()))
NEAR = RING - 1


def chunks_of(count):
    return [(k, start, VOCAB_CHUNK) for k in range(2) for start in range(0, count, VOCAB_CHUNK)]


def head_copies(heads, vocab, sems):
    count = heads[0].shape[0]
    for c, (k, start, size) in enumerate(chunks_of(count)):
        src = heads[k].at[pl.ds(start, size)]
        yield pltpu.make_async_copy(src, vocab.at[pl.ds(k * count + start, size)], sems.at[c])


def statistics(place, tokens, vocab, copies):
    width = vocab.shape[-1]
    lanes = EXTRA
    weight = lax.broadcasted_iota(jnp.int32, (EXTRA, lanes), 0)
    weight = jnp.where(weight == 0, 65536, jnp.where(weight == 1, 256, jnp.where(weight == 2, 1, 0)))
    weight = weight.astype(jnp.float32).astype(jnp.bfloat16)
    labels = tokens[:, pl.ds(width, EXTRA)]
    labels = jnp.dot(labels, weight, preferred_element_type=jnp.float32).astype(jnp.int32)
    lane = lax.broadcasted_iota(jnp.int32, labels.shape, 1)
    peak = jnp.full(labels.shape, -jnp.inf, jnp.float32)
    mass = jnp.zeros(labels.shape, jnp.float32)
    hit = jnp.zeros(labels.shape, jnp.float32)
    count = vocab.shape[0] // 2
    for copy, (k, start, size) in zip(copies, chunks_of(count)):
        copy.wait()
        words = vocab[pl.ds(k * count + start, size)]
        logits = lax.dot_general(
            tokens[:, pl.ds(0, width)], words, CONTRACT, preferred_element_type=jnp.float32
        )
        label = labels - (place[12 + k] + start)
        parts = [logits[:, i * lanes : (i + 1) * lanes] for i in range(size // lanes)]
        top = functools.reduce(jnp.maximum, parts, peak)
        mass = mass * jnp.exp(peak - top)
        for i, value in enumerate(parts):
            mass += jnp.exp(value - top)
            hit += jnp.where(label == lane + i * lanes, value, 0.0)
        peak = top
    top = jnp.max(peak, axis=1, keepdims=True)
    value = top + jnp.log(jnp.sum(mass * jnp.exp(peak - top), axis=1, keepdims=True))
    return value, jnp.sum(hit, axis=1, keepdims=True)


def near_kernel(place, *refs):
    a, b, c, heads, out, rows, vocab, row_sem, head_sems = (
        refs[:3], refs[3:6], refs[6:9], refs[9:11], *refs[11:],
    )
    part = a[0].shape[-1]
    near = pl.ds(0, NEAR)
    pairs = []
    for i in range(NEAR):
        pairs.append((a[i].at[near, near], rows.at[i, :, :, :, pl.ds(0, part)]))
        pairs.append((c[i].at[near, near], rows.at[:, :, i, :, pl.ds(2 * part, part)]))
        pairs.append((b[i].at[near, near], rows.at[:, i, :, :, pl.ds(part, part)]))
    for src, dst in pairs:
        pltpu.make_async_copy(src, dst, row_sem).start()
    copies = list(head_copies(heads, vocab, head_sems))
    for copy in copies:
        copy.start()
    pltpu.make_async_copy(rows, rows, row_sem).wait()
    count = out.shape[1]
    tokens = rows.reshape(count, 3 * part)
    for k, column in enumerate(statistics(place, tokens, vocab, copies)):
        out[k] = jnp.broadcast_to(column, out.shape[1:])


def far_kernel(place, *refs):
    a, b, c, heads, near_stats, pipe_of, out = refs[:4], refs[4:8], refs[8:12], refs[12:14], *refs[14:17]
    groups, rows, vocab, values_at, hits_at, row_sems, head_sems = refs[17:20], *refs[20:]
    part = a[0].shape[-1]
    shard = a[0].shape[-2]
    near, last = pl.ds(0, NEAR), RING - 1
    low, mid, high = pl.ds(0, part), pl.ds(part, part), pl.ds(2 * part, part)
    by_x, by_z, by_y = groups
    pairs = [(0, a[last], by_x.at[:, :, :, low]), (1, b[last].at[near], by_z.at[:, :, :, mid])]
    pairs += [(2, c[last].at[near, near], by_y.at[:, :, :, high])]
    for i in range(RING):
        pairs.append((0, b[i].at[last], by_x.at[i, :, :, mid]))
        pairs.append((0, c[i].at[last], by_x.at[:, i, :, high]))
        pairs.append((1, c[i].at[near, last], by_z.at[:, i, :, high]))
    for i in range(NEAR):
        pairs.append((1, a[i].at[last], by_z.at[i, :, :, low]))
        pairs.append((2, a[i].at[near, last], by_y.at[i, :, :, low]))
        pairs.append((2, b[i].at[near, last], by_y.at[:, i, :, mid]))
    for g, src, dst in pairs:
        pltpu.make_async_copy(src, dst, row_sems.at[g]).start()
    copies = list(head_copies(heads, vocab, head_sems))
    for copy in copies:
        copy.start()
    start = 0
    for g, group in enumerate(groups):
        size = group.shape[0] * group.shape[1] * shard
        pltpu.make_async_copy(group, group, row_sems.at[g]).wait()
        rows[pl.ds(start, size)] = group[...].reshape(size, 3 * part)
        start += size
    lanes = EXTRA
    far = [(last, z, y) for z in range(RING) for y in range(RING)]
    far += [(x, last, y) for x in range(NEAR) for y in range(RING)]
    far += [(x, z, last) for x in range(NEAR) for z in range(NEAR)]
    close = [(x, z, y) for x in range(NEAR) for z in range(NEAR) for y in range(NEAR)]

    def member(x, z, y):
        return (place[x] * RING + place[RING + z]) * RING + place[2 * RING + y]

    for k, column in enumerate(statistics(place, rows, vocab, copies)):
        to = (values_at, hits_at)[k]
        for s, spot in enumerate(far):
            to[member(*spot)] = jnp.broadcast_to(column[s * shard : (s + 1) * shard], (shard, lanes))
        for s, spot in enumerate(close):
            to[member(*spot)] = near_stats[k, s * shard : (s + 1) * shard]

    row = lax.broadcasted_iota(jnp.int32, (lanes, lanes), 0)
    diagonal = row == lax.broadcasted_iota(jnp.int32, (lanes, lanes), 1)
    count = pipe_of.shape[0]
    per = lanes // shard

    def lines(columns):
        square = [columns[g * per : (g + 1) * per].reshape(lanes, lanes) for g in range(count)]
        return [jnp.sum(jnp.where(diagonal, s, 0.0), axis=0, keepdims=True) for s in square]

    values = lines(values_at)
    found = jnp.concatenate(lines(hits_at), axis=0)
    coarse, fine = split(found)
    lane = lax.broadcasted_iota(jnp.int32, (1, lanes), 1)
    tail = jnp.zeros((1, lanes), jnp.float32)
    for p in range(PIPES):
        mine = pipe_of[...] == p
        for k, term in enumerate((coarse, fine)):
            value = jnp.sum(jnp.where(mine, term, 0.0), keepdims=True)
            tail = jnp.where(lane == shard + k * PIPES + p, value, tail)
    for k in range(per):
        rolled = found if k == 0 else pltpu.roll(found, lanes - k * shard, 1)
        for r in range(count):
            out[r * per + k, :, count * lanes :] = jnp.where(lane < shard, rolled[r : r + 1], tail)
    for g in range(count):
        for d in range(out.shape[0]):
            out[d, :, g * lanes : (g + 1) * lanes] = values[g]


def near_losses(place, near, head, other):
    shard, part = near[0][0].shape[-2:]
    count, width = head.shape
    chunks = len(chunks_of(count))
    tokens = NEAR**3 * shard
    hbm = pl.BlockSpec(memory_space=pltpu.HBM)
    return pl.pallas_call(
        near_kernel,
        in_specs=[pl.BlockSpec(memory_space=pltpu.SMEM)] + [hbm] * 11,
        out_specs=pl.BlockSpec(memory_space=pltpu.VMEM),
        out_shape=jax.ShapeDtypeStruct((2, tokens, EXTRA), jnp.float32),
        scratch_shapes=[
            pltpu.VMEM((NEAR, NEAR, NEAR, shard, 3 * part), jnp.bfloat16),
            pltpu.VMEM((2 * count, width), jnp.bfloat16),
            pltpu.SemaphoreType.DMA(()),
            pltpu.SemaphoreType.DMA((chunks,)),
        ],
        compiler_params=pltpu.CompilerParams(vmem_limit_bytes=40 * 1024 * 1024),
        cost_estimate=pl.CostEstimate(
            flops=4 * tokens * width * count, bytes_accessed=20 << 20, transcendentals=2 * tokens * count
        ),
        name="near_losses",
    )(place, *sum(near, []), head, other)


def far_losses(place, near, far, head, other, near_stats, pipe_of):
    shard, part = near[0][0].shape[-2:]
    count, width = head.shape
    chunks = len(chunks_of(count))
    members = RING**3
    tokens = members * shard
    hbm = pl.BlockSpec(memory_space=pltpu.HBM)
    vmem = pl.BlockSpec(memory_space=pltpu.VMEM)
    groups = ((RING, RING), (NEAR, RING), (NEAR, NEAR))
    return pl.pallas_call(
        far_kernel,
        in_specs=[pl.BlockSpec(memory_space=pltpu.SMEM)] + [hbm] * 14 + [vmem] * 2,
        out_specs=vmem,
        out_shape=jax.ShapeDtypeStruct((members, 1, tokens + EXTRA), jnp.float32),
        scratch_shapes=[pltpu.VMEM(g + (shard, 3 * part), jnp.bfloat16) for g in groups]
        + [
            pltpu.VMEM((tokens - NEAR**3 * shard, 3 * part), jnp.bfloat16),
            pltpu.VMEM((2 * count, width), jnp.bfloat16),
            pltpu.VMEM((members, shard, EXTRA), jnp.float32),
            pltpu.VMEM((members, shard, EXTRA), jnp.float32),
            pltpu.SemaphoreType.DMA((3,)),
            pltpu.SemaphoreType.DMA((chunks,)),
        ],
        compiler_params=pltpu.CompilerParams(vmem_limit_bytes=48 * 1024 * 1024),
        name="far_losses",
    )(place, *sum(([*n, f] for n, f in zip(near, far)), []), head, other, near_stats, pipe_of)


def finish_kernel(mine, stats, pipe_of, losses, pipes):
    lanes = losses.shape[1]
    tokens = pipe_of.shape[1]
    local = stats[:, :, :tokens]
    top = jnp.max(local, axis=0)
    total = top + jnp.log(jnp.sum(jnp.exp(local - top[None]), axis=0))
    tail = jnp.sum(stats[:, :, tokens:], axis=0)
    own = jnp.zeros((1, lanes), jnp.float32)
    for g in range(tokens // lanes):
        own = jnp.where(mine[0] == g, total[:, g * lanes : (g + 1) * lanes], own)
    losses[...] = pltpu.roll(own, mine[1], 1) - tail
    lane = lax.broadcasted_iota(jnp.int32, (1, lanes), 1)
    sums = []
    for k, part in enumerate(split(total)):
        row = jnp.zeros((1, lanes), jnp.float32)
        for p in range(PIPES):
            value = jnp.sum(jnp.where(pipe_of[...] == p, part, 0.0), keepdims=True)
            row = jnp.where(lane == p, value, row)
        sums.append(row - pltpu.roll(tail, lanes - mine[2] - k * PIPES, 1))
    pipes[...] = sums[0] + sums[1]


def finish(mine, stats, pipe_of):
    vmem = pl.BlockSpec(memory_space=pltpu.VMEM)
    return pl.pallas_call(
        finish_kernel,
        in_specs=[pl.BlockSpec(memory_space=pltpu.SMEM), vmem, vmem],
        out_specs=[vmem, vmem],
        out_shape=[jax.ShapeDtypeStruct((1, 128), jnp.float32)] * 2,
        name="finish",
    )(mine, stats, pipe_of)


def shards(hidden, norm_gain, head, targets, route):
    rows = hidden.shape[0]
    x, core, z, y = (lax.axis_index(a) for a in ALL)
    devices = lax.axis_size(ALL)
    pipes = lax.axis_size((X, CORE))
    count = head.shape[0]
    other = lax.ppermute(head, CORE, [(0, 1), (1, 0)])
    near, far = gather(*normalize(hidden, norm_gain, targets))
    own = lax.axis_index(ALL)
    partner = ((x * 2 + 1 - core) * RING + z) * RING + y
    at = [sender(axis, offset) for axis in (X, Z, Y) for offset in OFFSETS]
    place = jnp.stack([*at, own * count, partner * count]).astype(jnp.int32)
    near_stats = near_losses(place, near, head, other)
    members = lax.axis_size(CLASS)
    lanes = 128
    pipe_of = lax.dynamic_index_in_dim(route.reshape(RING, 2, RING * RING), core, 1, keepdims=False)
    pipe_of = jnp.repeat(pipe_of.reshape(members), rows).reshape(members * rows // lanes, lanes)
    stats = far_losses(place, near, far, head, other, near_stats, pipe_of)
    stats = lax.all_to_all(stats, CLASS, 0, 0, tiled=True)
    first = lax.axis_index(CLASS) * rows
    mine = jnp.stack([first // lanes, (lanes - first % lanes) % lanes, rows]).astype(jnp.int32)
    losses, sums = finish(mine, stats, pipe_of.reshape(1, members * rows))
    sums = (sums + lax.ppermute(sums, CORE, [(0, 1), (1, 0)])) / (rows * devices // pipes)
    return (losses[0, :rows], sums[0, :pipes])


def solution(mesh):
    torus = Mesh(mesh.devices.reshape(RING, 2, RING, RING), ALL)
    return jax.shard_map(
        shards,
        mesh=torus,
        in_specs=(P(ALL, None), P(), P(ALL, None), P(ALL), P()),
        out_specs=(P(ALL), P()),
        check_vma=False,
    )
```

```python
import functools

import jax
import jax.numpy as jnp
from jax import lax
from jax.experimental import pallas as pl
from jax.experimental.pallas import tpu as pltpu
from jax.sharding import Mesh
from jax.sharding import PartitionSpec as P


X, CORE, Z, Y = "dp_0", "dp_1", "pp_0", "pp_1"
ALL = (X, CORE, Z, Y)
CLASS = (X, Z, Y)
RING = 4
OFFSETS = (0, -1, 1, 2)
ORDERS = ((Y, Z, X), (Y, X, Z), (Z, X, Y))
EXTRA = 128
VOCAB_CHUNK = 512


def shift(x, axis, offset):
    pairs = []
    for i in range(RING):
        for core in range(2):
            to = (i - offset * (1 - 2 * core)) % RING
            pairs.append((i * 2 + core, to * 2 + core) if axis == X else (core * RING + i, core * RING + to))
    return lax.ppermute(x, (X, CORE) if axis == X else (CORE, axis), pairs)


def sender(axis, offset):
    return (lax.axis_index(axis) + offset * (1 - 2 * lax.axis_index(CORE))) % RING


def norm_kernel(targets, hidden, gain, *parts):
    rows, width = hidden.shape
    wide = hidden[...].astype(jnp.float32)
    factor = lax.rsqrt(jnp.mean(wide * wide, axis=1, keepdims=True) + 1e-05)
    normed = (wide * factor * gain[...]).astype(jnp.bfloat16)
    row = lax.broadcasted_iota(jnp.int32, (rows, EXTRA), 0)
    lane = lax.broadcasted_iota(jnp.int32, (rows, EXTRA), 1)
    ids = jnp.zeros((rows, EXTRA), jnp.int32)
    for i in range(rows):
        ids = jnp.where(row == i, targets[i], ids)
    digit = jnp.where(lane == 0, ids >> 16, jnp.where(lane == 1, (ids >> 8) & 255, ids & 255))
    digit = jnp.where(lane < 3, digit, 0).astype(jnp.float32).astype(jnp.bfloat16)
    part = (width + EXTRA) // 3
    parts[0][...] = normed[:, : 2 * part]
    parts[1][:, : part - EXTRA] = normed[:, 2 * part :]
    parts[1][:, part - EXTRA :] = digit


def normalize(hidden, gain, targets):
    rows, width = hidden.shape
    part = (width + EXTRA) // 3
    vmem = pl.BlockSpec(memory_space=pltpu.VMEM)
    return pl.pallas_call(
        norm_kernel,
        in_specs=[pl.BlockSpec(memory_space=pltpu.SMEM), vmem, vmem],
        out_specs=[vmem] * 2,
        out_shape=[jax.ShapeDtypeStruct((rows, 2 * part), jnp.bfloat16), jax.ShapeDtypeStruct((rows, part), jnp.bfloat16)],
        name="normalize",
    )(targets, hidden, gain.reshape(1, width))


def ring(x, axis):
    return [x] + [shift(x, axis, offset) for offset in OFFSETS[1:]]


def gather(both, third):
    part = third.shape[1]
    both = ring(both, ORDERS[0][0])
    third = ring(third, ORDERS[2][0])
    parts = [
        jnp.stack([x[:, :part] for x in both]),
        jnp.stack([x[:, part:] for x in both]),
        jnp.stack(third),
    ]
    parts = [jnp.stack(ring(x, order[1])) for x, order in zip(parts, ORDERS)]
    near = []
    for x, order in zip(parts, ORDERS):
        left = shift(x, order[2], OFFSETS[1])
        right = shift(x, order[2], OFFSETS[2])
        near.append([x, left, right])
    far = [shift(n[1], order[2], OFFSETS[1]) for n, order in zip(near, ORDERS)]
    return near, far


PIPES = 8


def split(x):
    coarse = jnp.floor(x * (1.0 / 256.0)) * 256.0
    return coarse, x - coarse


CONTRACT = (((1,), (1,)), ((), ()))
NEAR = RING - 1


def chunks_of(count):
    return [(k, start, VOCAB_CHUNK) for k in range(2) for start in range(0, count, VOCAB_CHUNK)]


def head_copies(heads, vocab, sems):
    count = heads[0].shape[0]
    for c, (k, start, size) in enumerate(chunks_of(count)):
        src = heads[k].at[pl.ds(start, size)]
        yield pltpu.make_async_copy(src, vocab.at[pl.ds(k * count + start, size)], sems.at[c])


def statistics(place, tokens, vocab, copies):
    width = vocab.shape[-1]
    lanes = EXTRA
    weight = lax.broadcasted_iota(jnp.int32, (EXTRA, lanes), 0)
    weight = jnp.where(weight == 0, 65536, jnp.where(weight == 1, 256, jnp.where(weight == 2, 1, 0)))
    weight = weight.astype(jnp.float32).astype(jnp.bfloat16)
    labels = tokens[:, pl.ds(width, EXTRA)]
    labels = jnp.dot(labels, weight, preferred_element_type=jnp.float32).astype(jnp.int32)
    lane = lax.broadcasted_iota(jnp.int32, labels.shape, 1)
    peak = jnp.full(labels.shape, -jnp.inf, jnp.float32)
    mass = jnp.zeros(labels.shape, jnp.float32)
    hit = jnp.zeros(labels.shape, jnp.float32)
    count = vocab.shape[0] // 2
    for copy, (k, start, size) in zip(copies, chunks_of(count)):
        copy.wait()
        words = vocab[pl.ds(k * count + start, size)]
        logits = lax.dot_general(
            tokens[:, pl.ds(0, width)], words, CONTRACT, preferred_element_type=jnp.float32
        )
        label = labels - (place[12 + k] + start)
        parts = [logits[:, i * lanes : (i + 1) * lanes] for i in range(size // lanes)]
        top = functools.reduce(jnp.maximum, parts, peak)
        mass = mass * jnp.exp(peak - top)
        for i, value in enumerate(parts):
            mass += jnp.exp(value - top)
            hit += jnp.where(label == lane + i * lanes, value, 0.0)
        peak = top
    top = jnp.max(peak, axis=1, keepdims=True)
    value = top + jnp.log(jnp.sum(mass * jnp.exp(peak - top), axis=1, keepdims=True))
    return value, jnp.sum(hit, axis=1, keepdims=True)


def near_kernel(place, *refs):
    a, b, c, heads, out, rows, vocab, row_sem, head_sems = (
        refs[:3], refs[3:6], refs[6:9], refs[9:11], *refs[11:],
    )
    part = a[0].shape[-1]
    near = pl.ds(0, NEAR)
    pairs = []
    for i in range(NEAR):
        pairs.append((a[i].at[near, near], rows.at[i, :, :, :, pl.ds(0, part)]))
        pairs.append((c[i].at[near, near], rows.at[:, :, i, :, pl.ds(2 * part, part)]))
        pairs.append((b[i].at[near, near], rows.at[:, i, :, :, pl.ds(part, part)]))
    for src, dst in pairs:
        pltpu.make_async_copy(src, dst, row_sem).start()
    copies = list(head_copies(heads, vocab, head_sems))
    for copy in copies:
        copy.start()
    pltpu.make_async_copy(rows, rows, row_sem).wait()
    count = out.shape[1]
    tokens = rows.reshape(count, 3 * part)
    for k, column in enumerate(statistics(place, tokens, vocab, copies)):
        out[k] = jnp.broadcast_to(column, out.shape[1:])


def far_kernel(place, *refs):
    a, b, c, heads, near_stats, pipe_of, out = refs[:4], refs[4:8], refs[8:12], refs[12:14], *refs[14:17]
    groups, rows, vocab, values_at, hits_at, row_sems, head_sems = refs[17:20], *refs[20:]
    part = a[0].shape[-1]
    shard = a[0].shape[-2]
    near, last = pl.ds(0, NEAR), RING - 1
    low, mid, high = pl.ds(0, part), pl.ds(part, part), pl.ds(2 * part, part)
    by_x, by_z, by_y = groups
    pairs = [(0, a[last], by_x.at[:, :, :, low]), (1, b[last].at[near], by_z.at[:, :, :, mid])]
    pairs += [(2, c[last].at[near, near], by_y.at[:, :, :, high])]
    for i in range(RING):
        pairs.append((0, b[i].at[last], by_x.at[i, :, :, mid]))
        pairs.append((0, c[i].at[last], by_x.at[:, i, :, high]))
        pairs.append((1, c[i].at[near, last], by_z.at[:, i, :, high]))
    for i in range(NEAR):
        pairs.append((1, a[i].at[last], by_z.at[i, :, :, low]))
        pairs.append((2, a[i].at[near, last], by_y.at[i, :, :, low]))
        pairs.append((2, b[i].at[near, last], by_y.at[:, i, :, mid]))
    for g, src, dst in pairs:
        pltpu.make_async_copy(src, dst, row_sems.at[g]).start()
    copies = list(head_copies(heads, vocab, head_sems))
    for copy in copies:
        copy.start()
    start = 0
    for g, group in enumerate(groups):
        size = group.shape[0] * group.shape[1] * shard
        pltpu.make_async_copy(group, group, row_sems.at[g]).wait()
        rows[pl.ds(start, size)] = group[...].reshape(size, 3 * part)
        start += size
    lanes = EXTRA
    far = [(last, z, y) for z in range(RING) for y in range(RING)]
    far += [(x, last, y) for x in range(NEAR) for y in range(RING)]
    far += [(x, z, last) for x in range(NEAR) for z in range(NEAR)]
    close = [(x, z, y) for x in range(NEAR) for z in range(NEAR) for y in range(NEAR)]

    def member(x, z, y):
        return (place[x] * RING + place[RING + z]) * RING + place[2 * RING + y]

    for k, column in enumerate(statistics(place, rows, vocab, copies)):
        to = (values_at, hits_at)[k]
        for s, spot in enumerate(far):
            to[member(*spot)] = jnp.broadcast_to(column[s * shard : (s + 1) * shard], (shard, lanes))
        for s, spot in enumerate(close):
            to[member(*spot)] = near_stats[k, s * shard : (s + 1) * shard]

    row = lax.broadcasted_iota(jnp.int32, (lanes, lanes), 0)
    diagonal = row == lax.broadcasted_iota(jnp.int32, (lanes, lanes), 1)
    count = pipe_of.shape[0]
    per = lanes // shard

    def lines(columns):
        square = [columns[g * per : (g + 1) * per].reshape(lanes, lanes) for g in range(count)]
        return [jnp.sum(jnp.where(diagonal, s, 0.0), axis=0, keepdims=True) for s in square]

    values = lines(values_at)
    found = jnp.concatenate(lines(hits_at), axis=0)
    coarse, fine = split(found)
    lane = lax.broadcasted_iota(jnp.int32, (1, lanes), 1)
    tail = jnp.zeros((1, lanes), jnp.float32)
    for p in range(PIPES):
        mine = pipe_of[...] == p
        for k, term in enumerate((coarse, fine)):
            value = jnp.sum(jnp.where(mine, term, 0.0), keepdims=True)
            tail = jnp.where(lane == shard + k * PIPES + p, value, tail)
    for k in range(per):
        rolled = found if k == 0 else pltpu.roll(found, lanes - k * shard, 1)
        for r in range(count):
            out[r * per + k, :, count * lanes :] = jnp.where(lane < shard, rolled[r : r + 1], tail)
    for g in range(count):
        for d in range(out.shape[0]):
            out[d, :, g * lanes : (g + 1) * lanes] = values[g]


def near_losses(place, near, head, other):
    shard, part = near[0][0].shape[-2:]
    count, width = head.shape
    chunks = len(chunks_of(count))
    tokens = NEAR**3 * shard
    hbm = pl.BlockSpec(memory_space=pltpu.HBM)
    return pl.pallas_call(
        near_kernel,
        in_specs=[pl.BlockSpec(memory_space=pltpu.SMEM)] + [hbm] * 11,
        out_specs=pl.BlockSpec(memory_space=pltpu.VMEM),
        out_shape=jax.ShapeDtypeStruct((2, tokens, EXTRA), jnp.float32),
        scratch_shapes=[
            pltpu.VMEM((NEAR, NEAR, NEAR, shard, 3 * part), jnp.bfloat16),
            pltpu.VMEM((2 * count, width), jnp.bfloat16),
            pltpu.SemaphoreType.DMA(()),
            pltpu.SemaphoreType.DMA((chunks,)),
        ],
        compiler_params=pltpu.CompilerParams(vmem_limit_bytes=40 * 1024 * 1024),
        cost_estimate=pl.CostEstimate(
            flops=4 * tokens * width * count, bytes_accessed=20 << 20, transcendentals=2 * tokens * count
        ),
        name="near_losses",
    )(place, *sum(near, []), head, other)


def far_losses(place, near, far, head, other, near_stats, pipe_of):
    shard, part = near[0][0].shape[-2:]
    count, width = head.shape
    chunks = len(chunks_of(count))
    members = RING**3
    tokens = members * shard
    hbm = pl.BlockSpec(memory_space=pltpu.HBM)
    vmem = pl.BlockSpec(memory_space=pltpu.VMEM)
    groups = ((RING, RING), (NEAR, RING), (NEAR, NEAR))
    return pl.pallas_call(
        far_kernel,
        in_specs=[pl.BlockSpec(memory_space=pltpu.SMEM)] + [hbm] * 14 + [vmem] * 2,
        out_specs=vmem,
        out_shape=jax.ShapeDtypeStruct((members, 1, tokens + EXTRA), jnp.float32),
        scratch_shapes=[pltpu.VMEM(g + (shard, 3 * part), jnp.bfloat16) for g in groups]
        + [
            pltpu.VMEM((tokens - NEAR**3 * shard, 3 * part), jnp.bfloat16),
            pltpu.VMEM((2 * count, width), jnp.bfloat16),
            pltpu.VMEM((members, shard, EXTRA), jnp.float32),
            pltpu.VMEM((members, shard, EXTRA), jnp.float32),
            pltpu.SemaphoreType.DMA((3,)),
            pltpu.SemaphoreType.DMA((chunks,)),
        ],
        compiler_params=pltpu.CompilerParams(vmem_limit_bytes=48 * 1024 * 1024),
        name="far_losses",
    )(place, *sum(([*n, f] for n, f in zip(near, far)), []), head, other, near_stats, pipe_of)


def finish_kernel(mine, stats, pipe_of, losses, pipes):
    lanes = losses.shape[1]
    tokens = pipe_of.shape[1]
    local = stats[:, :, :tokens]
    top = jnp.max(local, axis=0)
    total = top + jnp.log(jnp.sum(jnp.exp(local - top[None]), axis=0))
    tail = jnp.sum(stats[:, :, tokens:], axis=0)
    own = jnp.zeros((1, lanes), jnp.float32)
    for g in range(tokens // lanes):
        own = jnp.where(mine[0] == g, total[:, g * lanes : (g + 1) * lanes], own)
    losses[...] = pltpu.roll(own, mine[1], 1) - tail
    lane = lax.broadcasted_iota(jnp.int32, (1, lanes), 1)
    sums = []
    for k, part in enumerate(split(total)):
        row = jnp.zeros((1, lanes), jnp.float32)
        for p in range(PIPES):
            value = jnp.sum(jnp.where(pipe_of[...] == p, part, 0.0), keepdims=True)
            row = jnp.where(lane == p, value, row)
        sums.append(row - pltpu.roll(tail, lanes - mine[2] - k * PIPES, 1))
    pipes[...] = sums[0] + sums[1]


def finish(mine, stats, pipe_of):
    vmem = pl.BlockSpec(memory_space=pltpu.VMEM)
    return pl.pallas_call(
        finish_kernel,
        in_specs=[pl.BlockSpec(memory_space=pltpu.SMEM), vmem, vmem],
        out_specs=[vmem, vmem],
        out_shape=[jax.ShapeDtypeStruct((1, 128), jnp.float32)] * 2,
        name="finish",
    )(mine, stats, pipe_of)


def shards(hidden, norm_gain, head, targets, route):
    rows = hidden.shape[0]
    x, core, z, y = (lax.axis_index(a) for a in ALL)
    devices = lax.axis_size(ALL)
    pipes = lax.axis_size((X, CORE))
    count = head.shape[0]
    other = lax.ppermute(head, CORE, [(0, 1), (1, 0)])
    near, far = gather(*normalize(hidden, norm_gain, targets))
    own = lax.axis_index(ALL)
    partner = ((x * 2 + 1 - core) * RING + z) * RING + y
    at = [sender(axis, offset) for axis in (X, Z, Y) for offset in OFFSETS]
    place = jnp.stack([*at, own * count, partner * count]).astype(jnp.int32)
    near_stats = near_losses(place, near, head, other)
    members = lax.axis_size(CLASS)
    lanes = 128
    pipe_of = lax.dynamic_index_in_dim(route.reshape(RING, 2, RING * RING), core, 1, keepdims=False)
    pipe_of = jnp.repeat(pipe_of.reshape(members), rows).reshape(members * rows // lanes, lanes)
    stats = far_losses(place, near, far, head, other, near_stats, pipe_of)
    stats = lax.all_to_all(stats, CLASS, 0, 0, tiled=True)
    first = lax.axis_index(CLASS) * rows
    mine = jnp.stack([first // lanes, (lanes - first % lanes) % lanes, rows]).astype(jnp.int32)
    losses, sums = finish(mine, stats, pipe_of.reshape(1, members * rows))
    sums = (sums + lax.ppermute(sums, CORE, [(0, 1), (1, 0)])) / (rows * devices // pipes)
    return (losses[0, :rows], sums[0, :pipes])


def solution(mesh):
    torus = Mesh(mesh.devices.reshape(RING, 2, RING, RING), ALL)
    return jax.shard_map(
        shards,
        mesh=torus,
        in_specs=(P(ALL, None), P(), P(ALL, None), P(ALL), P()),
        out_specs=(P(ALL), P()),
        check_vma=False,
    )
```
